32 devices in a mesh: grp: 2 (over x), dom: 16 (over z, y, core).
Axes of the slice: x: 2, y: 2, z: 4, core: 2. Of those that a mesh axis runs over, the one named last changes fastest.
Arguments:
- surplus: float32 [48, 64, 4096], P('grp', None, 'dom'), may hold values from -40 to 40
- levels: int32 [48, 3], P('grp'), may hold values from 0 to 3
Outputs:
- updated: float32 [48, 64, 4096], P('grp', None, 'dom')
- coefficients: float32 [48], replicated
The draws below stay inside these ranges and needn't reach their ends.
All inputs are finite; a program needn't handle non-finite values.
Results may differ from the reference program's by a relative error of at most 0.0003.
Values sent between devices are 32-bit elements; how exact they have to be, the bound alone decides.
A program may use at most 64 MiB of HBM per device.

```python
import math
import jax
import jax.numpy as jnp
from jax import lax

GRIDS = 48
SUBSP = 64
NC = 4096


def draw_surplus(key, part):
    keys = jax.random.split(jax.random.fold_in(key, 11), 4)
    index = jnp.arange(SUBSP, dtype=jnp.int32)
    level_sum = (index // 16 + index // 4 % 4 + index % 4).astype(jnp.float32)
    position = jnp.arange(NC, dtype=jnp.float32) / float(max(NC - 1, 1))
    common = jax.random.normal(keys[0], (SUBSP, NC), jnp.float32)
    single = jax.random.normal(keys[1], (GRIDS, SUBSP, NC), jnp.float32)
    gains = jnp.exp(jax.random.uniform(keys[2], (GRIDS, SUBSP, 1), jnp.float32, math.log(0.5), math.log(2.0)))
    spread = jnp.exp(jax.random.uniform(keys[3], (GRIDS, SUBSP, 1), jnp.float32, math.log(0.4), math.log(1.2)))
    envelope = 3.0 ** position / math.sqrt(3.0)
    amplitude = 1.5 * 10.0 ** (-level_sum / 9.0)
    values = envelope[None, None, :] * amplitude[None, :, None] * (gains * common[None] + spread * single)
    return jnp.clip(values, -40.0, 40.0).astype(jnp.float32)


def set_ends(result, own_key, smallest, high):
    dims = result.shape
    index_at = [jax.random.randint(jax.random.fold_in(own_key, axis), (), 0, dims[axis]) for axis in range(len(dims))]
    result = result.at[tuple(index_at)].set(smallest)
    longest = dims.index(max(dims))
    index_at[longest] = (index_at[longest] + 1) % dims[longest]
    return result.at[tuple(index_at)].set(high)


def setup_inputs(seed: int = 0) -> dict:
    arg_keys = jax.random.split(jax.random.key(seed), 3)
    return {
        "surplus": draw_surplus(jax.random.fold_in(arg_keys[2], 71), 0),
        "levels": set_ends(jax.random.randint(arg_keys[1], (GRIDS, 3), 0, 4), jax.random.fold_in(arg_keys[1], 1), 0, 3).astype(jnp.int32),
    }


def owned(levels, count):
    indices = jnp.arange(count, dtype=jnp.int32)
    digits = jnp.stack([indices // 16, indices // 4 % 4, indices % 4])
    return jnp.all(digits[None] <= levels[:, :, None], axis=1).astype(jnp.float32)

def solve_weights(gram_matrix):
    number = gram_matrix.shape[0]
    diagonal_part = jnp.diagonal(gram_matrix) + 1e-06
    scaling = 1.0 / jnp.sqrt(diagonal_part)
    system = scaling[:, None] * gram_matrix * scaling[None, :] + 0.1 * jnp.eye(number, dtype=jnp.float32)
    factor = jnp.linalg.cholesky(system)
    target = jnp.sqrt(diagonal_part)[:, None]
    halfway = lax.linalg.triangular_solve(factor, target, left_side=True, lower=True)
    weights = lax.linalg.triangular_solve(factor, halfway, left_side=True, lower=True, transpose_a=True)
    return scaling * weights[:, 0]

def reference(surplus, levels):
    owners = owned(levels, SUBSP)
    masked = surplus * owners[:, :, None]
    flattened = masked.reshape(GRIDS, -1)
    gram_matrix = jnp.dot(flattened.astype(jnp.float32), flattened.T.astype(jnp.float32), precision=lax.Precision.HIGHEST, preferred_element_type=jnp.float32)
    coefficients = solve_weights(gram_matrix)
    combined = jnp.tensordot(coefficients, masked, axes=1, precision=lax.Precision.HIGHEST)
    updated = owners[:, :, None] * combined[None]
    return (updated, coefficients)
```

```python
import functools

import jax
import jax.numpy as jnp
from jax import lax
from jax.experimental import pallas as pl
from jax.experimental.pallas import tpu as pltpu
from jax.sharding import PartitionSpec as P

MESH = pl.DeviceIdType.MESH
ROWS = 8
BLOCK = 16
PIECES = 2
SPREAD = 4
SLOT = 32
STEP = 128
VMEM_BYTES = 24 * 1024 * 1024
F32 = jnp.float32


def radices_of(size):
    out = []
    while size > 1:
        for r in (4, 2, 3, 5, 7, size):
            if size % r == 0:
                out.append(r)
                size //= r
                break
    return out


def digits_of(sub):
    return (sub // 16).astype(F32), lax.rem(sub // 4, 4).astype(F32), lax.rem(sub, 4).astype(F32)


def split3(x):
    hi = x.astype(jnp.bfloat16)
    rest = x - hi.astype(F32)
    mid = rest.astype(jnp.bfloat16)
    lo = (rest - mid.astype(F32)).astype(jnp.bfloat16)
    return jnp.concatenate([hi, mid, lo], axis=0)


def kernel(groups, radices, local, subs, surplus, levels, comb_out, coef_out, lev_out, *scratch):
    stages = len(radices)
    (xb, lev, lbc, prod, cbuf, local_sem, lev_send, lev_recv, x_send, x_recv, c_send, c_recv) = scratch[:12]
    slots = scratch[12:12 + stages]
    s_send = scratch[12 + stages:12 + 2 * stages]
    s_recv = scratch[12 + 2 * stages:12 + 3 * stages]
    grids = groups * local
    half = xb.shape[-1]
    chunks = subs // ROWS
    g = lax.axis_index("grp")
    d = lax.axis_index("dom")

    members = []
    stride = 1
    for t, r in enumerate(radices):
        digit = lax.rem(d // stride, r)
        base = d - digit * stride
        if t == 0:
            n = groups * r
            mine = g * r + digit
            device = functools.partial(lambda b, r_, q: (q // r_, b + lax.rem(q, r_)), base, r)
        else:
            n = r
            mine = digit
            device = functools.partial(lambda b, st, q: (g, b + q * st), base, stride)
        members.append((n, mine, device))
        stride *= r

    barrier = pltpu.get_barrier_semaphore()
    count = 0
    for n, mine, device in members:
        for k in range(1, n):
            q = lax.rem(mine + k, n)
            pl.semaphore_signal(barrier, inc=1, device_id=device(q), device_id_type=MESH)
            count += 1

    own_cells = pl.ds(pl.multiple_of(g * half, half), half)
    own_copy = pltpu.make_async_copy(
        surplus.at[:, :, own_cells], xb.at[pl.ds(g * local, local)], local_sem
    )
    own_copy.start()
    pl.semaphore_wait(barrier, count)

    def lev_copy(k):
        q = lax.rem(g + k, groups)
        return pltpu.make_async_remote_copy(
            src_ref=levels, dst_ref=lev.at[g], send_sem=lev_send.at[k], recv_sem=lev_recv.at[g],
            device_id=(q, d), device_id_type=MESH,
        )

    def x_copy(k, ch):
        q = lax.rem(g + k, groups)
        rows = pl.ds(pl.multiple_of(ch * ROWS, ROWS), ROWS)
        return pltpu.make_async_remote_copy(
            src_ref=surplus.at[:, rows, pl.ds(pl.multiple_of(q * half, half), half)],
            dst_ref=xb.at[pl.ds(g * local, local), rows],
            send_sem=x_send.at[k, ch], recv_sem=x_recv.at[g, ch],
            device_id=(q, d), device_id_type=MESH,
        )

    def x_arrival(k, ch):
        q = lax.rem(g + k, groups)
        rows = pl.ds(pl.multiple_of(ch * ROWS, ROWS), ROWS)
        block = xb.at[pl.ds(q * local, local), rows]
        return pltpu.make_async_remote_copy(
            src_ref=block, dst_ref=block, send_sem=x_send.at[k, ch], recv_sem=x_recv.at[q, ch],
            device_id=(q, d), device_id_type=MESH,
        )

    for k in range(1, groups):
        lev_copy(k).start()
    for ch in range(chunks):
        for k in range(1, groups):
            x_copy(k, ch).start()

    lev[g] = levels[...]
    for k in range(1, groups):
        q = lax.rem(g + k, groups)
        pltpu.make_async_remote_copy(
            src_ref=lev.at[q], dst_ref=lev.at[q], send_sem=lev_send.at[k], recv_sem=lev_recv.at[q],
            device_id=(q, d), device_id_type=MESH,
        ).wait_recv()
    lev_eye = lax.broadcasted_iota(jnp.int32, (local, local), 0) == lax.broadcasted_iota(
        jnp.int32, (local, local), 1
    )
    for h in range(groups):
        for axis in range(3):
            lev_row = lev[h, axis:axis + 1, :].astype(F32)
            lev_col = jnp.sum(jnp.where(lev_eye, lev_row, 0.0), axis=1, keepdims=True)
            lbc[axis, pl.ds(h * local, local), :] = jnp.broadcast_to(lev_col, (local, 128))
    lev_out[...] = lbc[:, pl.ds(pl.multiple_of(g * local, 8), local), :]
    prod[...] = jnp.zeros_like(prod)
    own_copy.wait()
    flat = xb.reshape(grids * subs, half)

    def gram_chunk(ch, carry):
        for k in range(1, groups):
            x_arrival(k, ch).wait_recv()
        lev0, lev1, lev2 = lbc[0], lbc[1], lbc[2]
        total = jnp.zeros(prod.shape, F32)
        for pair in range(0, ROWS, 2):
            parts = []
            for k in range(pair, pair + 2):
                s = ch * ROWS + k
                x = flat[pl.ds(s, grids, stride=subs), :]
                keep = (
                    (lev0 >= (s // 16).astype(F32))
                    & (lev1 >= lax.rem(s // 4, 4).astype(F32))
                    & (lev2 >= float(k % 4))
                )
                keep = jnp.concatenate([keep] * (half // 128), axis=1) if half > 128 else keep
                parts.append(jnp.where(keep, x, 0.0))
            y = split3(jnp.concatenate(parts, axis=1))
            total += lax.dot_general(y, y, (((1,), (1,)), ((), ())), preferred_element_type=F32)
        prod[...] += total
        return carry

    lax.fori_loop(0, chunks, gram_chunk, 0)

    part = prod[2 * grids:, :] + prod[grids:2 * grids, :] + prod[:grids, :]
    part = part[:, 2 * grids:] + part[:, grids:2 * grids] + part[:, :grids]
    value = jnp.concatenate([part, jnp.zeros((grids, 128 - grids), F32)], axis=1)
    fold = grids // 2
    value = value[:fold] + pltpu.roll(value[fold:], 64, 1)

    copies = []
    for t, (n, mine, device) in enumerate(members):
        buf, send, recv = slots[t], s_send[t], s_recv[t]
        buf[mine] = value
        for k in range(1, n):
            q = lax.rem(mine + k, n)
            copy = pltpu.make_async_remote_copy(
                src_ref=buf.at[mine], dst_ref=buf.at[mine], send_sem=send.at[k], recv_sem=recv.at[mine],
                device_id=device(q), device_id_type=MESH,
            )
            copy.start()
            copies.append(copy)
        for k in range(1, n):
            q = lax.rem(mine + k, n)
            pltpu.make_async_remote_copy(
                src_ref=buf.at[q], dst_ref=buf.at[q], send_sem=send.at[k], recv_sem=recv.at[q],
                device_id=device(q), device_id_type=MESH,
            ).wait_recv()
        value = buf[0]
        for q in range(1, n):
            value = value + buf[q]

    left = lax.broadcasted_iota(jnp.int32, (fold, 128), 1) < 64
    value = jnp.concatenate(
        [jnp.where(left, value, 0.0), jnp.where(left, pltpu.roll(value, 64, 1), 0.0)], axis=0
    )

    row = lax.broadcasted_iota(jnp.int32, (grids, 128), 0)
    col = lax.broadcasted_iota(jnp.int32, (grids, 128), 1)
    eye = row == col
    diag = jnp.where(eye, value, 0.0)
    diag_col = jnp.sum(diag, axis=1, keepdims=True) + 1e-06
    diag_row = jnp.sum(diag, axis=0, keepdims=True) + 1e-06
    scale_col = 1.0 / jnp.sqrt(diag_col)
    scale_row = 1.0 / jnp.sqrt(diag_row)
    system = scale_col * value * scale_row + jnp.where(eye, 0.1, 0.0)
    system = jnp.where(col == grids, jnp.sqrt(diag_col), jnp.where(col < grids, system, 0.0))
    for first in range(0, grids, BLOCK):
        width = min(BLOCK, grids - first)
        rows = [system[first + j:first + j + 1, :] for j in range(width)]
        cols = [
            jnp.broadcast_to(system[:, first + j:first + j + 1], (grids, 128)) for j in range(width)
        ]
        for j in range(width):
            k = first + j
            inverse = 1.0 / cols[j][k:k + 1, :]
            factor = jnp.where(row == k, 0.0, cols[j] * inverse)
            for m in range(j + 1, width):
                cols[m] = cols[m] - factor * cols[m][k:k + 1, :]
                rows[m] = rows[m] - factor[first + m:first + m + 1, :] * rows[j]
            system = system - factor * rows[j]
    final = jnp.sum(jnp.where(eye, system, 0.0), axis=1, keepdims=True)
    coef = scale_col * (system[:, grids:grids + 1] / final)
    coef_wide = jnp.broadcast_to(coef, (grids, 128))
    coef_out[...] = jnp.sum(jnp.where(eye, coef_wide, 0.0), axis=0, keepdims=True)[:, :grids]

    piece = subs // PIECES

    def c_copy(slot, k, p):
        block = cbuf.at[slot, pl.ds(p * piece, piece)]
        return pltpu.make_async_remote_copy(
            src_ref=block, dst_ref=block, send_sem=c_send.at[k, p], recv_sem=c_recv.at[slot, p],
            device_id=(lax.rem(g + k, groups), d), device_id_type=MESH,
        )

    for p in range(PIECES):
        sub = lax.broadcasted_iota(jnp.int32, (piece, half), 0) + p * piece
        dig0, dig1, dig2 = digits_of(sub)
        acc = jnp.zeros((piece, half), F32)
        for i in range(grids):
            keep = (
                (lbc[0, i:i + 1, 0:1] >= dig0)
                & (lbc[1, i:i + 1, 0:1] >= dig1)
                & (lbc[2, i:i + 1, 0:1] >= dig2)
            )
            acc += jnp.where(keep, coef_wide[i:i + 1, 0:1], 0.0) * xb[i, p * piece:(p + 1) * piece]
        cbuf[g, p * piece:(p + 1) * piece] = acc
        for k in range(1, groups):
            c_copy(g, k, p).start()
    for p in range(PIECES):
        for k in range(1, groups):
            c_copy(lax.rem(g + k, groups), k, p).wait_recv()
    for h in range(groups):
        comb_out[:, h * half:(h + 1) * half] = cbuf[h]

    for copy in copies:
        copy.wait_send()
    for k in range(1, groups):
        lev_copy(k).wait_send()
        for ch in range(chunks):
            x_copy(k, ch).wait_send()
        for p in range(PIECES):
            c_copy(g, k, p).wait_send()


def layout_of(groups, radices, g, d):
    members = []
    stride = 1
    for t, r in enumerate(radices):
        digit = lax.rem(d // stride, r)
        base = d - digit * stride
        if t == 0:
            n = groups * r
            mine = g * r + digit
            device = functools.partial(lambda b, r_, q: (q // r_, b + lax.rem(q, r_)), base, r)
        else:
            n = r
            mine = digit
            device = functools.partial(lambda b, st, q: (g, b + q * st), base, stride)
        members.append((n, mine, device))
        stride *= r
    return members


def spread_out(members, t, buf, send, recv, value):
    n, mine, device = members[t]
    buf[mine] = value
    copies = []
    for k in range(1, n):
        copy = pltpu.make_async_remote_copy(
            src_ref=buf.at[mine], dst_ref=buf.at[mine], send_sem=send.at[k], recv_sem=recv.at[mine],
            device_id=device(lax.rem(mine + k, n)), device_id_type=MESH,
        )
        copy.start()
        copies.append(copy)
    return copies


def gather_in(members, t, buf, send, recv):
    n, mine, device = members[t]
    for k in range(1, n):
        q = lax.rem(mine + k, n)
        pltpu.make_async_remote_copy(
            src_ref=buf.at[q], dst_ref=buf.at[q], send_sem=send.at[k], recv_sem=recv.at[q],
            device_id=device(q), device_id_type=MESH,
        ).wait_recv()


def total_of(buf, first, last):
    value = buf[first]
    for q in range(first + 1, last):
        value = value + buf[q]
    return value


def pack(square):
    local = square.shape[0]
    wide = jnp.concatenate([square, jnp.zeros((local, 128 - local), F32)], axis=1)
    out = wide[:8]
    for b in range(1, local // 8):
        out = out + pltpu.roll(wide[8 * b:8 * b + 8], SLOT * b, 1)
    return out


def unpack(packed, local):
    rows = [packed] + [pltpu.roll(packed, 128 - SLOT * b, 1) for b in range(1, local // 8)]
    wide = jnp.concatenate(rows, axis=0)
    return jnp.where(lax.broadcasted_iota(jnp.int32, (local, 128), 1) < local, wide, 0.0)


def folded(products, n):
    part = products[2 * n:, :] + products[n:2 * n, :] + products[:n, :]
    return part[:, 2 * n:] + part[:, n:2 * n] + part[:, :n]


def outer(a, b):
    return lax.dot_general(a, b, (((1,), (1,)), ((), ())), preferred_element_type=F32)


def count_dot(a, b):
    bf16 = jnp.bfloat16
    return jnp.dot(a.astype(bf16), b.astype(bf16), preferred_element_type=F32)


def below(n, m, flip):
    r = lax.broadcasted_iota(jnp.int32, (n, m), 0)
    c = lax.broadcasted_iota(jnp.int32, (n, m), 1)
    return jnp.where((r < c) if flip else (r > c), 1.0, 0.0)


def solve(value, grids):
    row = lax.broadcasted_iota(jnp.int32, (grids, 128), 0)
    col = lax.broadcasted_iota(jnp.int32, (grids, 128), 1)
    eye = row == col
    diag = jnp.where(eye, value, 0.0)
    diag_col = jnp.sum(diag, axis=1, keepdims=True) + 1e-06
    diag_row = jnp.sum(diag, axis=0, keepdims=True) + 1e-06
    scale_col = 1.0 / jnp.sqrt(diag_col)
    scale_row = 1.0 / jnp.sqrt(diag_row)
    system = scale_col * value * scale_row + jnp.where(eye, 0.1, 0.0)
    system = jnp.where(col == grids, jnp.sqrt(diag_col), jnp.where(col < grids, system, 0.0))
    for first in range(0, grids, BLOCK):
        width = min(BLOCK, grids - first)
        rows = [system[first + j:first + j + 1, :] for j in range(width)]
        cols = [
            jnp.broadcast_to(system[:, first + j:first + j + 1], (grids, 128)) for j in range(width)
        ]
        for j in range(width):
            k = first + j
            inverse = 1.0 / cols[j][k:k + 1, :]
            factor = jnp.where(row == k, 0.0, cols[j] * inverse)
            for m in range(j + 1, width):
                cols[m] = cols[m] - factor * cols[m][k:k + 1, :]
                rows[m] = rows[m] - factor[first + m:first + m + 1, :] * rows[j]
            system = system - factor * rows[j]
    final = jnp.sum(jnp.where(eye, system, 0.0), axis=1, keepdims=True)
    coef = scale_col * (system[:, grids:grids + 1] / final)
    return jnp.broadcast_to(coef, (grids, 128)), eye


def sparse_kernel(groups, radices, local, subs, cap, surplus, levels, comb_out, coef_out, lev_out, fits_out, *scratch):
    stages = len(radices)
    (xb, xp, xs, csend, crecv, posb, lev, lbc, prod, cross, cbuf, local_sem, lev_sem, x_send, x_recv, c_send,
     c_recv) = scratch[:17]
    rest = [scratch[17 + m * stages:17 + (m + 1) * stages] for m in range(6)]
    slots, s_send, s_recv, own_slots, o_send, o_recv = rest
    grids = groups * local
    half = xb.shape[-1]
    chunks = cap // STEP
    g = lax.axis_index("grp")
    d = lax.axis_index("dom")
    other = 1 - g
    members = layout_of(groups, radices, g, d)

    own_cells = pl.ds(pl.multiple_of(g * half, half), half)
    other_cells = pl.ds(pl.multiple_of(other * half, half), half)
    lev_load = pltpu.make_async_copy(levels, lev.at[g], local_sem.at[0])
    xp_load = pltpu.make_async_copy(surplus.at[:, :, other_cells], xp, local_sem.at[1])
    xb_load = pltpu.make_async_copy(surplus.at[:, :, own_cells], xb.at[pl.ds(g * local, local)], local_sem.at[2])
    lev_load.start()
    xp_load.start()
    xb_load.start()

    barrier = pltpu.get_barrier_semaphore()
    count = 0
    for n, mine, device in members:
        for k in range(1, n):
            pl.semaphore_signal(barrier, inc=1, device_id=device(lax.rem(mine + k, n)), device_id_type=MESH)
            count += 1

    lev_load.wait()
    lev_eye = lax.broadcasted_iota(jnp.int32, (local, local), 0) == lax.broadcasted_iota(
        jnp.int32, (local, local), 1
    )
    digits = digits_of(lax.broadcasted_iota(jnp.int32, (local, 128), 1))
    keep = jnp.ones((local, 128), F32)
    for axis in range(3):
        lev_row = lev[g, axis:axis + 1, :].astype(F32)
        lev_col = jnp.sum(jnp.where(lev_eye, lev_row, 0.0), axis=1, keepdims=True)
        wide = jnp.broadcast_to(lev_col, (local, 128))
        lev_out[axis] = wide
        keep = jnp.where(wide >= digits[axis], keep, 0.0)
    totals = count_dot(jnp.ones((local, local), F32), keep)
    pos = count_dot(below(local, local, False), keep) + count_dot(totals, below(128, 128, True))
    pos = jnp.where(keep > 0.0, pos, -1.0)
    pos_far = pltpu.roll(pos, 64, 1)
    own_count = jnp.sum(keep)

    low = lax.broadcasted_iota(jnp.int32, (1, 128), 1) < subs
    per = 128 // subs
    pos_rows = [jnp.where(low, pos[i:i + 1], pos_far[i + 1:i + 2]) for i in range(0, local, per)]

    xp_load.wait()
    flat_p = xp.reshape(local * subs, half)
    for i in range(0, local * subs, 256):
        x = flat_p[i:i + 256, :]
        hi = x.astype(jnp.bfloat16)
        left = x - hi.astype(F32)
        mid = left.astype(jnp.bfloat16)
        xs[i:i + 256, 0:half] = hi
        xs[i:i + 256, half:2 * half] = mid
        xs[i:i + 256, 2 * half:] = (left - mid.astype(F32)).astype(jnp.bfloat16)

    pl.semaphore_wait(barrier, count)
    lev_copy = pltpu.make_async_remote_copy(
        src_ref=lev.at[g], dst_ref=lev.at[g], send_sem=lev_sem.at[0], recv_sem=lev_sem.at[1],
        device_id=(other, d), device_id_type=MESH,
    )
    lev_copy.start()

    def x_copy(ch):
        rows = pl.ds(pl.multiple_of(ch * STEP, STEP), STEP)
        return pltpu.make_async_remote_copy(
            src_ref=csend.at[rows], dst_ref=crecv.at[rows], send_sem=x_send.at[ch], recv_sem=x_recv.at[ch],
            device_id=(other, d), device_id_type=MESH,
        )

    index = lax.broadcasted_iota(jnp.int32, (STEP, 128), 0).astype(F32)

    def send_chunk(ch, carry):
        want = index + (ch * STEP).astype(F32)
        acc = jnp.zeros((STEP, 3 * half), F32)
        for m in range(0, len(pos_rows), 2):
            picks = [jnp.where(want == p, 1.0, 0.0).astype(jnp.bfloat16) for p in pos_rows[m:m + 2]]
            acc += jnp.dot(
                jnp.concatenate(picks, axis=1), xs[m * 128:m * 128 + 256, :], preferred_element_type=F32
            )
        rows = pl.ds(pl.multiple_of(ch * STEP, STEP), STEP)
        csend[rows, :] = acc[:, :half] + acc[:, half:2 * half] + acc[:, 2 * half:]
        x_copy(ch).start()
        return carry

    lax.fori_loop(0, chunks, send_chunk, 0)

    xb_load.wait()
    dig_wide = digits_of(lax.broadcasted_iota(jnp.int32, (subs, 128), 0))
    for i in range(local):
        own = (
            (lev_out[0, i:i + 1, :] >= dig_wide[0])
            & (lev_out[1, i:i + 1, :] >= dig_wide[1])
            & (lev_out[2, i:i + 1, :] >= dig_wide[2])
        )
        for c in range(0, half, 128):
            xp[i, :, c:c + 128] = jnp.where(own, xp[i, :, c:c + 128], 0.0)
            xb[g * local + i, :, c:c + 128] = jnp.where(own, xb[g * local + i, :, c:c + 128], 0.0)
    flat = xb.reshape(grids * subs, half)

    prod[...] = jnp.zeros_like(prod)

    def own_gram(ch, carry):
        total = jnp.zeros(prod.shape, F32)
        for k in range(ROWS):
            s = ch * ROWS + k
            y = split3(jnp.concatenate(
                [flat_p[pl.ds(s, local, stride=subs), :], flat[pl.ds(g * local * subs + s, local, stride=subs), :]],
                axis=1,
            ))
            total += outer(y, y)
        prod[...] += total
        return carry

    lax.fori_loop(0, subs // ROWS, own_gram, 0)
    copies = spread_out(
        members, 0, own_slots[0], o_send[0], o_recv[0], pack(folded(prod[...], local))
    )

    lev_copy.wait_recv()
    digits = digits_of(lax.broadcasted_iota(jnp.int32, (subs, local), 0))
    keep = jnp.ones((subs, local), F32)
    for axis in range(3):
        keep = jnp.where(lev[other, axis:axis + 1, :].astype(F32) >= digits[axis], keep, 0.0)
    totals = count_dot(keep, jnp.ones((local, local), F32))
    pos = count_dot(below(subs, subs, False), totals) + count_dot(keep, below(local, local, True))
    pos = jnp.where(keep > 0.0, pos, -1.0)
    fits_out[0, 0] = jnp.where(jnp.maximum(own_count, jnp.sum(keep)) <= float(cap), 1, 0)
    for i in range(local):
        posb[i * subs:(i + 1) * subs, :] = jnp.broadcast_to(pos[:, i:i + 1], (subs, 128))
    xb[pl.ds(other * local, local)] = jnp.zeros((local, subs, half), F32)
    lane = lax.broadcasted_iota(jnp.int32, (256, STEP), 1).astype(F32)

    def place_chunk(ch, carry):
        x_copy(ch).wait_recv()
        rows = pl.ds(pl.multiple_of(ch * STEP, STEP), STEP)
        x = crecv[rows, :]
        hi = x.astype(jnp.bfloat16)
        left = x - hi.astype(F32)
        mid = left.astype(jnp.bfloat16)
        parts = jnp.concatenate([hi, mid, (left - mid.astype(F32)).astype(jnp.bfloat16)], axis=1)
        want = lane + (ch * STEP).astype(F32)
        for i in range(0, local * subs, 256):
            picks = jnp.where(want == posb[i:i + 256, :], 1.0, 0.0).astype(jnp.bfloat16)
            y = jnp.dot(picks, parts, preferred_element_type=F32)
            at = pl.ds(pl.multiple_of(other * local * subs + i, 256), 256)
            flat[at, :] += y[:, :half] + y[:, half:2 * half] + y[:, 2 * half:]
        return carry

    lax.fori_loop(0, chunks - 1, place_chunk, 0)
    gather_in(members, 0, own_slots[0], o_send[0], o_recv[0])
    half_n = members[0][0] // groups
    own_total = jnp.concatenate(
        [total_of(own_slots[0], 0, half_n), total_of(own_slots[0], half_n, 2 * half_n)], axis=0
    )
    if stages > 1:
        copies += spread_out(members, 1, own_slots[1], o_send[1], o_recv[1], own_total)
    lax.fori_loop(chunks - 1, chunks, place_chunk, 0)

    cross[...] = jnp.zeros_like(cross)

    def cross_gram(ch, carry):
        total = jnp.zeros(cross.shape, F32)
        for k in range(0, ROWS, 2):
            s = ch * ROWS + k
            sides = []
            for h in range(groups):
                sides.append(split3(jnp.concatenate(
                    [flat[pl.ds(h * local * subs + s + j, local, stride=subs), :] for j in range(2)], axis=1
                )))
            total += outer(sides[0], sides[1])
        cross[...] += total
        return carry

    lax.fori_loop(0, subs // ROWS, cross_gram, 0)
    value = pack(folded(cross[...], local))
    for t in range(stages):
        copies += spread_out(members, t, slots[t], s_send[t], s_recv[t], value)
        if t + 1 < stages:
            nxt = t + 1
            if t > 0:
                copies += spread_out(members, nxt, own_slots[nxt], o_send[nxt], o_recv[nxt], own_total)
            gather_in(members, nxt, own_slots[nxt], o_send[nxt], o_recv[nxt])
            own_total = total_of(own_slots[nxt], 0, members[nxt][0])
        gather_in(members, t, slots[t], s_send[t], s_recv[t])
        value = total_of(slots[t], 0, members[t][0])

    upper = unpack(value, local)
    square = jnp.concatenate([upper, jnp.zeros((128 - local, 128), F32)], axis=0)
    lower = square.T[:local]
    value = jnp.concatenate(
        [
            unpack(own_total[:8], local) + pltpu.roll(upper, local, 1),
            lower + pltpu.roll(unpack(own_total[8:], local), local, 1),
        ],
        axis=0,
    )
    coef_wide, eye = solve(value, grids)
    coef_out[...] = jnp.sum(jnp.where(eye, coef_wide, 0.0), axis=0, keepdims=True)[:, :grids]

    piece = subs // PIECES

    def c_copy(slot, p):
        block = cbuf.at[slot, pl.ds(p * piece, piece)]
        return pltpu.make_async_remote_copy(
            src_ref=block, dst_ref=block, send_sem=c_send.at[p], recv_sem=c_recv.at[p],
            device_id=(other, d), device_id_type=MESH,
        )

    for p in range(PIECES):
        acc = jnp.zeros((piece, half), F32)
        for i in range(grids):
            acc += coef_wide[i:i + 1, 0:1] * xb[i, p * piece:(p + 1) * piece]
        cbuf[g, p * piece:(p + 1) * piece] = acc
        c_copy(g, p).start()
    for p in range(PIECES):
        c_copy(other, p).wait_recv()
    for h in range(groups):
        comb_out[:, h * half:(h + 1) * half] = cbuf[h]

    for copy in copies:
        copy.wait_send()
    lev_copy.wait_send()
    for ch in range(chunks):
        x_copy(ch).wait_send()
    for p in range(PIECES):
        c_copy(g, p).wait_send()


def spread(combined, coef, lev, updated, coef_out, block, sems):
    local, subs, cells = updated.shape
    coef_out[...] = coef[...]
    dig0, dig1, dig2 = digits_of(lax.broadcasted_iota(jnp.int32, (subs, 128), 0))
    copies = []
    for i in range(local):
        keep = (lev[0, i:i + 1, :] >= dig0) & (lev[1, i:i + 1, :] >= dig1) & (lev[2, i:i + 1, :] >= dig2)
        for c in range(0, cells, 128):
            block[i, :, c:c + 128] = jnp.where(keep, combined[:, c:c + 128], 0.0)
        if (i + 1) % SPREAD == 0 or i + 1 == local:
            n = len(copies)
            part = pl.ds(n * SPREAD, i + 1 - n * SPREAD)
            copy = pltpu.make_async_copy(block.at[part], updated.at[part], sems.at[n])
            copy.start()
            copies.append(copy)
    for copy in copies:
        copy.wait()


def dense_call(groups, radices, surplus, levels, identity):
    local, subs, cells = surplus.shape
    grids = groups * local
    half = cells // groups
    sizes = [groups * r if t == 0 else r for t, r in enumerate(radices)]
    dma = pltpu.SemaphoreType.DMA
    chunks = subs // ROWS
    return pl.pallas_call(
        functools.partial(kernel, groups, radices, local, subs),
        out_shape=(
            jax.ShapeDtypeStruct((subs, cells), F32),
            jax.ShapeDtypeStruct((1, grids), F32),
            jax.ShapeDtypeStruct((3, local, 128), F32),
        ),
        in_specs=[pl.BlockSpec(memory_space=pltpu.HBM), pl.BlockSpec(memory_space=pltpu.VMEM)],
        out_specs=tuple(pl.BlockSpec(memory_space=pltpu.VMEM) for _ in range(3)),
        scratch_shapes=[
            pltpu.VMEM((grids, subs, half), F32),
            pltpu.VMEM((groups, 3, local), jnp.int32),
            pltpu.VMEM((3, grids, 128), F32),
            pltpu.VMEM((3 * grids, 3 * grids), F32),
            pltpu.VMEM((groups, subs, half), F32),
            dma(()), dma((groups,)), dma((groups,)),
            dma((groups, chunks)), dma((groups, chunks)), dma((groups, PIECES)), dma((groups, PIECES)),
        ]
        + [pltpu.VMEM((n, grids // 2, 128), F32) for n in sizes]
        + [dma((n,)) for n in sizes]
        + [dma((n,)) for n in sizes],
        compiler_params=pltpu.CompilerParams(
            collective_id=identity, has_side_effects=True, vmem_limit_bytes=VMEM_BYTES
        ),
    )(surplus, levels)


def sparse_call(groups, radices, surplus, levels, identity):
    local, subs, cells = surplus.shape
    grids = groups * local
    half = cells // groups
    cap = local * subs // 3 // STEP * STEP
    sizes = [groups * r if t == 0 else r for t, r in enumerate(radices)]
    dma = pltpu.SemaphoreType.DMA
    return pl.pallas_call(
        functools.partial(sparse_kernel, groups, radices, local, subs, cap),
        out_shape=(
            jax.ShapeDtypeStruct((subs, cells), F32),
            jax.ShapeDtypeStruct((1, grids), F32),
            jax.ShapeDtypeStruct((3, local, 128), F32),
            jax.ShapeDtypeStruct((1, 1), jnp.int32),
        ),
        in_specs=[pl.BlockSpec(memory_space=pltpu.HBM), pl.BlockSpec(memory_space=pltpu.HBM)],
        out_specs=tuple(pl.BlockSpec(memory_space=pltpu.VMEM) for _ in range(3))
        + (pl.BlockSpec(memory_space=pltpu.SMEM),),
        scratch_shapes=[
            pltpu.VMEM((grids, subs, half), F32),
            pltpu.VMEM((local, subs, half), F32),
            pltpu.VMEM((local * subs, 3 * half), jnp.bfloat16),
            pltpu.VMEM((cap, half), F32),
            pltpu.VMEM((cap, half), F32),
            pltpu.VMEM((local * subs, 128), F32),
            pltpu.VMEM((groups, 3, local), jnp.int32),
            pltpu.VMEM((3, grids, 128), F32),
            pltpu.VMEM((3 * local, 3 * local), F32),
            pltpu.VMEM((3 * local, 3 * local), F32),
            pltpu.VMEM((groups, subs, half), F32),
            dma((3,)), dma((2,)), dma((cap // STEP,)), dma((cap // STEP,)), dma((PIECES,)), dma((PIECES,)),
        ]
        + [pltpu.VMEM((n, 8, 128), F32) for n in sizes]
        + [dma((n,)) for n in sizes]
        + [dma((n,)) for n in sizes]
        + [pltpu.VMEM((n, 8 if t == 0 else 16, 128), F32) for t, n in enumerate(sizes)]
        + [dma((n,)) for n in sizes]
        + [dma((n,)) for n in sizes],
        compiler_params=pltpu.CompilerParams(
            collective_id=identity, has_side_effects=True, vmem_limit_bytes=VMEM_BYTES
        ),
    )(surplus, levels)


def shards(groups, domains, surplus, levels):
    local, subs, cells = surplus.shape
    grids = groups * local
    radices = radices_of(domains)
    flipped = levels.T
    *found, fits = sparse_call(groups, radices, surplus, flipped, 0)
    combined, coefficients, lev_wide = lax.cond(
        fits[0, 0] == 1,
        lambda *kept: tuple(kept[2:]),
        lambda *kept: tuple(dense_call(groups, radices, kept[0], kept[1], 1)),
        surplus, flipped, *found,
    )
    updated, coefficients = pl.pallas_call(
        spread,
        out_shape=(
            jax.ShapeDtypeStruct((local, subs, cells), F32),
            jax.ShapeDtypeStruct((1, grids), F32),
        ),
        in_specs=[pl.BlockSpec(memory_space=pltpu.VMEM)] * 3,
        out_specs=(pl.BlockSpec(memory_space=pl.ANY), pl.BlockSpec(memory_space=pltpu.VMEM)),
        scratch_shapes=[pltpu.VMEM((local, subs, cells), F32), pltpu.SemaphoreType.DMA((-(-local // SPREAD),))],
        compiler_params=pltpu.CompilerParams(vmem_limit_bytes=VMEM_BYTES),
    )(combined, coefficients, lev_wide)
    return (updated, coefficients.reshape(grids))


def solution(mesh):
    placed = (P("grp", None, "dom"), P("grp", None))
    return jax.shard_map(
        functools.partial(shards, mesh.shape["grp"], mesh.shape["dom"]),
        mesh=mesh, in_specs=placed, out_specs=(P("grp", None, "dom"), P()), check_vma=False,
    )
```

```python
import functools

import jax
import jax.numpy as jnp
from jax import lax
from jax.experimental import pallas as pl
from jax.experimental.pallas import tpu as pltpu
from jax.sharding import PartitionSpec as P

MESH = pl.DeviceIdType.MESH
ROWS = 8
BLOCK = 16
PIECES = 2
SPREAD = 4
SLOT = 32
STEP = 128
EARLY = 1
BAND = 384
VMEM_BYTES = 32 * 1024 * 1024
F32 = jnp.float32


def radices_of(size):
    out = []
    while size > 1:
        for r in (4, 2, 3, 5, 7, size):
            if size % r == 0:
                out.append(r)
                size //= r
                break
    return out


def digits_of(sub):
    return (sub // 16).astype(F32), lax.rem(sub // 4, 4).astype(F32), lax.rem(sub, 4).astype(F32)


def split3(x):
    hi = x.astype(jnp.bfloat16)
    rest = x - hi.astype(F32)
    mid = rest.astype(jnp.bfloat16)
    lo = (rest - mid.astype(F32)).astype(jnp.bfloat16)
    return jnp.concatenate([hi, mid, lo], axis=0)


def kernel(groups, radices, local, subs, surplus, levels, comb_out, coef_out, lev_out, *scratch):
    stages = len(radices)
    (xb, lev, lbc, prod, cbuf, local_sem, lev_send, lev_recv, x_send, x_recv, c_send, c_recv) = scratch[:12]
    slots = scratch[12:12 + stages]
    s_send = scratch[12 + stages:12 + 2 * stages]
    s_recv = scratch[12 + 2 * stages:12 + 3 * stages]
    grids = groups * local
    half = xb.shape[-1]
    chunks = subs // ROWS
    g = lax.axis_index("grp")
    d = lax.axis_index("dom")

    members = []
    stride = 1
    for t, r in enumerate(radices):
        digit = lax.rem(d // stride, r)
        base = d - digit * stride
        if t == 0:
            n = groups * r
            mine = g * r + digit
            device = functools.partial(lambda b, r_, q: (q // r_, b + lax.rem(q, r_)), base, r)
        else:
            n = r
            mine = digit
            device = functools.partial(lambda b, st, q: (g, b + q * st), base, stride)
        members.append((n, mine, device))
        stride *= r

    barrier = pltpu.get_barrier_semaphore()
    count = 0
    for n, mine, device in members:
        for k in range(1, n):
            q = lax.rem(mine + k, n)
            pl.semaphore_signal(barrier, inc=1, device_id=device(q), device_id_type=MESH)
            count += 1

    own_cells = pl.ds(pl.multiple_of(g * half, half), half)
    own_copy = pltpu.make_async_copy(
        surplus.at[:, :, own_cells], xb.at[pl.ds(g * local, local)], local_sem
    )
    own_copy.start()
    pl.semaphore_wait(barrier, count)

    def lev_copy(k):
        q = lax.rem(g + k, groups)
        return pltpu.make_async_remote_copy(
            src_ref=levels, dst_ref=lev.at[g], send_sem=lev_send.at[k], recv_sem=lev_recv.at[g],
            device_id=(q, d), device_id_type=MESH,
        )

    def x_copy(k, ch):
        q = lax.rem(g + k, groups)
        rows = pl.ds(pl.multiple_of(ch * ROWS, ROWS), ROWS)
        return pltpu.make_async_remote_copy(
            src_ref=surplus.at[:, rows, pl.ds(pl.multiple_of(q * half, half), half)],
            dst_ref=xb.at[pl.ds(g * local, local), rows],
            send_sem=x_send.at[k, ch], recv_sem=x_recv.at[g, ch],
            device_id=(q, d), device_id_type=MESH,
        )

    def x_arrival(k, ch):
        q = lax.rem(g + k, groups)
        rows = pl.ds(pl.multiple_of(ch * ROWS, ROWS), ROWS)
        block = xb.at[pl.ds(q * local, local), rows]
        return pltpu.make_async_remote_copy(
            src_ref=block, dst_ref=block, send_sem=x_send.at[k, ch], recv_sem=x_recv.at[q, ch],
            device_id=(q, d), device_id_type=MESH,
        )

    for k in range(1, groups):
        lev_copy(k).start()
    for ch in range(chunks):
        for k in range(1, groups):
            x_copy(k, ch).start()

    lev[g] = levels[...]
    for k in range(1, groups):
        q = lax.rem(g + k, groups)
        pltpu.make_async_remote_copy(
            src_ref=lev.at[q], dst_ref=lev.at[q], send_sem=lev_send.at[k], recv_sem=lev_recv.at[q],
            device_id=(q, d), device_id_type=MESH,
        ).wait_recv()
    lev_eye = lax.broadcasted_iota(jnp.int32, (local, local), 0) == lax.broadcasted_iota(
        jnp.int32, (local, local), 1
    )
    for h in range(groups):
        for axis in range(3):
            lev_row = lev[h, axis:axis + 1, :].astype(F32)
            lev_col = jnp.sum(jnp.where(lev_eye, lev_row, 0.0), axis=1, keepdims=True)
            lbc[axis, pl.ds(h * local, local), :] = jnp.broadcast_to(lev_col, (local, 128))
    lev_out[...] = lbc[:, pl.ds(pl.multiple_of(g * local, 8), local), :]
    prod[...] = jnp.zeros_like(prod)
    own_copy.wait()
    flat = xb.reshape(grids * subs, half)

    def gram_chunk(ch, carry):
        for k in range(1, groups):
            x_arrival(k, ch).wait_recv()
        lev0, lev1, lev2 = lbc[0], lbc[1], lbc[2]
        total = jnp.zeros(prod.shape, F32)
        for pair in range(0, ROWS, 2):
            parts = []
            for k in range(pair, pair + 2):
                s = ch * ROWS + k
                x = flat[pl.ds(s, grids, stride=subs), :]
                keep = (
                    (lev0 >= (s // 16).astype(F32))
                    & (lev1 >= lax.rem(s // 4, 4).astype(F32))
                    & (lev2 >= float(k % 4))
                )
                keep = jnp.concatenate([keep] * (half // 128), axis=1) if half > 128 else keep
                parts.append(jnp.where(keep, x, 0.0))
            y = split3(jnp.concatenate(parts, axis=1))
            total += lax.dot_general(y, y, (((1,), (1,)), ((), ())), preferred_element_type=F32)
        prod[...] += total
        return carry

    lax.fori_loop(0, chunks, gram_chunk, 0)

    part = prod[2 * grids:, :] + prod[grids:2 * grids, :] + prod[:grids, :]
    part = part[:, 2 * grids:] + part[:, grids:2 * grids] + part[:, :grids]
    value = jnp.concatenate([part, jnp.zeros((grids, 128 - grids), F32)], axis=1)
    fold = grids // 2
    value = value[:fold] + pltpu.roll(value[fold:], 64, 1)

    copies = []
    for t, (n, mine, device) in enumerate(members):
        buf, send, recv = slots[t], s_send[t], s_recv[t]
        buf[mine] = value
        for k in range(1, n):
            q = lax.rem(mine + k, n)
            copy = pltpu.make_async_remote_copy(
                src_ref=buf.at[mine], dst_ref=buf.at[mine], send_sem=send.at[k], recv_sem=recv.at[mine],
                device_id=device(q), device_id_type=MESH,
            )
            copy.start()
            copies.append(copy)
        for k in range(1, n):
            q = lax.rem(mine + k, n)
            pltpu.make_async_remote_copy(
                src_ref=buf.at[q], dst_ref=buf.at[q], send_sem=send.at[k], recv_sem=recv.at[q],
                device_id=device(q), device_id_type=MESH,
            ).wait_recv()
        value = buf[0]
        for q in range(1, n):
            value = value + buf[q]

    left = lax.broadcasted_iota(jnp.int32, (fold, 128), 1) < 64
    value = jnp.concatenate(
        [jnp.where(left, value, 0.0), jnp.where(left, pltpu.roll(value, 64, 1), 0.0)], axis=0
    )

    row = lax.broadcasted_iota(jnp.int32, (grids, 128), 0)
    col = lax.broadcasted_iota(jnp.int32, (grids, 128), 1)
    eye = row == col
    diag = jnp.where(eye, value, 0.0)
    diag_col = jnp.sum(diag, axis=1, keepdims=True) + 1e-06
    diag_row = jnp.sum(diag, axis=0, keepdims=True) + 1e-06
    scale_col = 1.0 / jnp.sqrt(diag_col)
    scale_row = 1.0 / jnp.sqrt(diag_row)
    system = scale_col * value * scale_row + jnp.where(eye, 0.1, 0.0)
    system = jnp.where(col == grids, jnp.sqrt(diag_col), jnp.where(col < grids, system, 0.0))
    for first in range(0, grids, BLOCK):
        width = min(BLOCK, grids - first)
        rows = [system[first + j:first + j + 1, :] for j in range(width)]
        cols = [
            jnp.broadcast_to(system[:, first + j:first + j + 1], (grids, 128)) for j in range(width)
        ]
        for j in range(width):
            k = first + j
            inverse = 1.0 / cols[j][k:k + 1, :]
            factor = jnp.where(row == k, 0.0, cols[j] * inverse)
            for m in range(j + 1, width):
                cols[m] = cols[m] - factor * cols[m][k:k + 1, :]
                rows[m] = rows[m] - factor[first + m:first + m + 1, :] * rows[j]
            system = system - factor * rows[j]
    final = jnp.sum(jnp.where(eye, system, 0.0), axis=1, keepdims=True)
    coef = scale_col * (system[:, grids:grids + 1] / final)
    coef_wide = jnp.broadcast_to(coef, (grids, 128))
    coef_out[...] = jnp.sum(jnp.where(eye, coef_wide, 0.0), axis=0, keepdims=True)[:, :grids]

    piece = subs // PIECES

    def c_copy(slot, k, p):
        block = cbuf.at[slot, pl.ds(p * piece, piece)]
        return pltpu.make_async_remote_copy(
            src_ref=block, dst_ref=block, send_sem=c_send.at[k, p], recv_sem=c_recv.at[slot, p],
            device_id=(lax.rem(g + k, groups), d), device_id_type=MESH,
        )

    for p in range(PIECES):
        sub = lax.broadcasted_iota(jnp.int32, (piece, half), 0) + p * piece
        dig0, dig1, dig2 = digits_of(sub)
        acc = jnp.zeros((piece, half), F32)
        for i in range(grids):
            keep = (
                (lbc[0, i:i + 1, 0:1] >= dig0)
                & (lbc[1, i:i + 1, 0:1] >= dig1)
                & (lbc[2, i:i + 1, 0:1] >= dig2)
            )
            acc += jnp.where(keep, coef_wide[i:i + 1, 0:1], 0.0) * xb[i, p * piece:(p + 1) * piece]
        cbuf[g, p * piece:(p + 1) * piece] = acc
        for k in range(1, groups):
            c_copy(g, k, p).start()
    for p in range(PIECES):
        for k in range(1, groups):
            c_copy(lax.rem(g + k, groups), k, p).wait_recv()
    for h in range(groups):
        comb_out[:, h * half:(h + 1) * half] = cbuf[h]

    for copy in copies:
        copy.wait_send()
    for k in range(1, groups):
        lev_copy(k).wait_send()
        for ch in range(chunks):
            x_copy(k, ch).wait_send()
        for p in range(PIECES):
            c_copy(g, k, p).wait_send()


def split3_rows(x):
    hi = x.astype(jnp.bfloat16).astype(F32)
    rest = x - hi
    mid = rest.astype(jnp.bfloat16).astype(F32)
    return jnp.concatenate([hi, mid, rest - mid], axis=0).astype(jnp.bfloat16)


def layout_of(groups, radices, g, d):
    members = []
    stride = 1
    for t, r in enumerate(radices):
        digit = lax.rem(d // stride, r)
        base = d - digit * stride
        if t == 0:
            n = groups * r
            mine = g * r + digit
            device = functools.partial(lambda b, r_, q: (q // r_, b + lax.rem(q, r_)), base, r)
        else:
            n = r
            mine = digit
            device = functools.partial(lambda b, st, q: (g, b + q * st), base, stride)
        members.append((n, mine, device))
        stride *= r
    return members


def spread_out(members, t, buf, send, recv, value):
    n, mine, device = members[t]
    buf[mine] = value
    copies = []
    for k in range(1, n):
        copy = pltpu.make_async_remote_copy(
            src_ref=buf.at[mine], dst_ref=buf.at[mine], send_sem=send.at[k], recv_sem=recv.at[mine],
            device_id=device(lax.rem(mine + k, n)), device_id_type=MESH,
        )
        copy.start()
        copies.append(copy)
    return copies


def gather_in(members, t, buf, send, recv):
    n, mine, device = members[t]
    for k in range(1, n):
        q = lax.rem(mine + k, n)
        pltpu.make_async_remote_copy(
            src_ref=buf.at[q], dst_ref=buf.at[q], send_sem=send.at[k], recv_sem=recv.at[q],
            device_id=device(q), device_id_type=MESH,
        ).wait_recv()


def total_of(buf, first, last):
    value = buf[first]
    for q in range(first + 1, last):
        value = value + buf[q]
    return value


def pack(square):
    local = square.shape[0]
    wide = jnp.concatenate([square, jnp.zeros((local, 128 - local), F32)], axis=1)
    out = wide[:8]
    for b in range(1, local // 8):
        out = out + pltpu.roll(wide[8 * b:8 * b + 8], SLOT * b, 1)
    return out


def unpack(packed, local):
    rows = [packed] + [pltpu.roll(packed, 128 - SLOT * b, 1) for b in range(1, local // 8)]
    wide = jnp.concatenate(rows, axis=0)
    return jnp.where(lax.broadcasted_iota(jnp.int32, (local, 128), 1) < local, wide, 0.0)


def folded(products, n):
    part = products[2 * n:, :] + products[n:2 * n, :] + products[:n, :]
    return part[:, 2 * n:] + part[:, n:2 * n] + part[:, :n]


def outer(a, b):
    return lax.dot_general(a, b, (((1,), (1,)), ((), ())), preferred_element_type=F32)


def count_dot(a, b):
    bf16 = jnp.bfloat16
    return jnp.dot(a.astype(bf16), b.astype(bf16), preferred_element_type=F32)


def below(n, m, flip):
    r = lax.broadcasted_iota(jnp.int32, (n, m), 0)
    c = lax.broadcasted_iota(jnp.int32, (n, m), 1)
    return jnp.where((r < c) if flip else (r > c), 1.0, 0.0)


def solve(value, grids):
    row = lax.broadcasted_iota(jnp.int32, (grids, 128), 0)
    col = lax.broadcasted_iota(jnp.int32, (grids, 128), 1)
    eye = row == col
    diag = jnp.where(eye, value, 0.0)
    diag_col = jnp.sum(diag, axis=1, keepdims=True) + 1e-06
    diag_row = jnp.sum(diag, axis=0, keepdims=True) + 1e-06
    scale_col = 1.0 / jnp.sqrt(diag_col)
    scale_row = 1.0 / jnp.sqrt(diag_row)
    system = scale_col * value * scale_row + jnp.where(eye, 0.1, 0.0)
    system = jnp.where(col == grids, jnp.sqrt(diag_col), jnp.where(col < grids, system, 0.0))
    for first in range(0, grids, BLOCK):
        width = min(BLOCK, grids - first)
        rows = [system[first + j:first + j + 1, :] for j in range(width)]
        cols = [
            jnp.broadcast_to(system[:, first + j:first + j + 1], (grids, 128)) for j in range(width)
        ]
        for j in range(width):
            k = first + j
            inverse = 1.0 / cols[j][k:k + 1, :]
            factor = jnp.where(row == k, 0.0, cols[j] * inverse)
            for m in range(j + 1, width):
                cols[m] = cols[m] - factor * cols[m][k:k + 1, :]
                rows[m] = rows[m] - factor[first + m:first + m + 1, :] * rows[j]
            system = system - factor * rows[j]
    final = jnp.sum(jnp.where(eye, system, 0.0), axis=1, keepdims=True)
    coef = scale_col * (system[:, grids:grids + 1] / final)
    return jnp.broadcast_to(coef, (grids, 128)), eye


def parts_of(x):
    hi = x.astype(jnp.bfloat16)
    left = x - hi.astype(F32)
    mid = left.astype(jnp.bfloat16)
    return hi, mid, (left - mid.astype(F32)).astype(jnp.bfloat16)


def places_of(keep, across):
    n, m = keep.shape
    if across:
        totals = count_dot(jnp.ones((n, n), F32), keep)
        pos = count_dot(below(n, n, False), keep) + count_dot(totals, below(m, m, True))
    else:
        totals = count_dot(keep, jnp.ones((m, m), F32))
        pos = count_dot(below(n, n, False), totals) + count_dot(keep, below(m, m, True))
    return jnp.where(keep > 0.0, pos, -1.0)


def sparse_kernel(groups, radices, local, subs, cap, surplus, levels, comb_out, coef_out, lev_out, fits_out, *scratch):
    stages = len(radices)
    (xh, xm, xs, ym, pm, csend, crecv, posm, lev, prod, cbuf, local_sem, m_sem, lev_sem, x_send,
     x_recv) = scratch[:16]
    rest = [scratch[16 + m * stages:16 + (m + 1) * stages] for m in range(6)]
    slots, s_send, s_recv, own_slots, o_send, o_recv = rest
    grids = groups * local
    half = xh.shape[-1]
    rows_all = local * subs
    chunks = cap // STEP
    bf16 = jnp.bfloat16
    g = lax.axis_index("grp")
    d = lax.axis_index("dom")
    other = 1 - g
    members = layout_of(groups, radices, g, d)

    cells = [pl.ds(pl.multiple_of(h * half, half), half) for h in (other, g)]
    lev_load = pltpu.make_async_copy(levels, lev.at[g], local_sem.at[2])
    lev_load.start()
    loads = [pltpu.make_async_copy(surplus.at[:, :, cells[h]], xh.at[h], local_sem.at[h]) for h in range(2)]
    for load in loads:
        load.start()
    turns = [
        pltpu.make_async_copy(surplus.at[i, :, cells[h]], xm.at[h, :, i, :], m_sem.at[h, i])
        for i in range(local) for h in range(2)
    ]
    for turn in turns:
        turn.start()

    barrier = pltpu.get_barrier_semaphore()
    count = 0
    for n, mine, device in members:
        for k in range(1, n):
            pl.semaphore_signal(barrier, inc=1, device_id=device(lax.rem(mine + k, n)), device_id_type=MESH)
            count += 1

    def lev_wide(h):
        eye = lax.broadcasted_iota(jnp.int32, (local, local), 0) == lax.broadcasted_iota(jnp.int32, (local, local), 1)
        out = []
        for axis in range(3):
            lev_row = lev[h, axis:axis + 1, :].astype(F32)
            lev_col = jnp.sum(jnp.where(eye, lev_row, 0.0), axis=1, keepdims=True)
            out.append(jnp.broadcast_to(lev_col, (local, 128)))
        return out

    def kept_by(wide):
        digits = digits_of(lax.broadcasted_iota(jnp.int32, (local, 128), 1))
        keep = jnp.ones((local, 128), F32)
        for axis in range(3):
            keep = jnp.where(wide[axis] >= digits[axis], keep, 0.0)
        return keep

    lev_load.wait()
    wide = lev_wide(g)
    for axis in range(3):
        lev_out[axis] = wide[axis]
    keep = kept_by(wide)
    own_count = jnp.sum(keep)
    pos = places_of(keep, True)
    pos_far = pltpu.roll(pos, 64, 1)
    low = lax.broadcasted_iota(jnp.int32, (1, 128), 1) < subs
    pos_rows = [jnp.where(low, pos[i:i + 1], pos_far[i + 1:i + 2]) for i in range(0, local, 128 // subs)]

    def split_half(h):
        flat = xh.at[h].reshape(rows_all, half)
        for i in range(0, rows_all, 256):
            for m, part in enumerate(parts_of(flat[i:i + 256, :])):
                xs[h, i:i + 256, m * half:(m + 1) * half] = part

    loads[0].wait()
    split_half(0)
    pl.semaphore_wait(barrier, count)
    lev_copy = pltpu.make_async_remote_copy(
        src_ref=lev.at[g], dst_ref=lev.at[g], send_sem=lev_sem.at[0], recv_sem=lev_sem.at[1],
        device_id=(other, d), device_id_type=MESH,
    )
    lev_copy.start()

    def x_copy(h, ch):
        rows = pl.ds(pl.multiple_of(ch * STEP, STEP), STEP)
        return pltpu.make_async_remote_copy(
            src_ref=csend.at[h, rows], dst_ref=crecv.at[h, rows], send_sem=x_send.at[h, ch], recv_sem=x_recv.at[h, ch],
            device_id=(other, d), device_id_type=MESH,
        )

    index = lax.broadcasted_iota(jnp.int32, (STEP, 128), 0).astype(F32)

    def gather_chunk(h, ch):
        want = index + (ch * STEP).astype(F32)
        acc = jnp.zeros((STEP, 3 * half), F32)
        for m in range(0, len(pos_rows), 2):
            picks = [jnp.where(want == p, 1.0, 0.0).astype(bf16) for p in pos_rows[m:m + 2]]
            acc += jnp.dot(
                jnp.concatenate(picks, axis=1), xs[h, m * 128:m * 128 + 256, :], preferred_element_type=F32
            )
        rows = pl.ds(pl.multiple_of(ch * STEP, STEP), STEP)
        csend[h, rows, :] = acc[:, :half] + acc[:, half:2 * half] + acc[:, 2 * half:]

    def send_chunk(h, ch, carry):
        gather_chunk(h, ch)
        x_copy(h, ch).start()
        return carry

    def hold_chunk(h, ch, carry):
        gather_chunk(h, ch)
        return carry

    lax.fori_loop(0, chunks, functools.partial(send_chunk, 0), 0)
    loads[1].wait()
    split_half(1)
    lax.fori_loop(0, EARLY, functools.partial(send_chunk, 1), 0)

    for turn in turns:
        turn.wait()
    prod[...] = jnp.zeros_like(prod)

    def own_gram(ch, carry):
        total = jnp.zeros(prod.shape, F32)
        for k in range(ROWS):
            s = ch * ROWS + k
            own = (
                (lev_out[0] >= (s // 16).astype(F32))
                & (lev_out[1] >= lax.rem(s // 4, 4).astype(F32))
                & (lev_out[2] >= float(k % 4))
            )
            own = jnp.concatenate([own] * (half // 128), axis=1) if half > 128 else own
            pair = [jnp.where(own, xm[h, s], 0.0) for h in range(2)]
            for h in range(2):
                xm[h, s] = pair[h]
            y = split3_rows(jnp.concatenate(pair, axis=1))
            ym[s] = y[:, half:]
            total += outer(y, y)
        prod[...] += total
        return carry

    lax.fori_loop(0, subs // ROWS, own_gram, 0)
    copies = spread_out(members, 0, own_slots[0], o_send[0], o_recv[0], pack(folded(prod[...], local)))
    lax.fori_loop(EARLY, chunks, functools.partial(hold_chunk, 1), 0)

    lev_copy.wait_recv()
    keep = kept_by(lev_wide(other))
    fits_out[0, 0] = jnp.where(jnp.maximum(own_count, jnp.sum(keep)) <= float(cap), 1, 0)
    pos = places_of(keep, True)
    for s in range(subs):
        posm[s * local:(s + 1) * local, :] = jnp.broadcast_to(pos[:, s:s + 1], (local, 128))

    def parts_at(h, first):
        return jnp.concatenate(parts_of(crecv[h, first:first + 256, :]), axis=1)

    def placed(where, first, parts, n):
        lane = lax.broadcasted_iota(jnp.int32, (n, 128), 1).astype(F32) + float(first)
        picks = [jnp.where(where == lane + float(c), 1.0, 0.0).astype(bf16) for c in range(0, 256, 128)]
        y = jnp.dot(jnp.concatenate(picks, axis=1), parts, preferred_element_type=F32)
        return y[:, :half] + y[:, half:2 * half] + y[:, 2 * half:]

    def arrive(h, first):
        for ch in range(first // STEP, (first + 256) // STEP):
            x_copy(h, ch).wait_recv()

    last = cap - 256
    for first in range(0, last, 256):
        arrive(0, first)
        parts = parts_at(0, first)

        for at in range(0, rows_all, BAND):
            y = placed(posm[at:at + BAND, :], first, parts, BAND)
            pm[1, at:at + BAND, :] = y if first == 0 else pm[1, at:at + BAND, :] + y

    arrive(0, last)
    parts = parts_at(0, last)
    total = jnp.zeros((3 * local, 3 * local), F32)
    for at in range(0, rows_all, BAND):
        y = placed(posm[at:at + BAND, :], last, parts, BAND)
        if last > 0:
            y = y + pm[1, at:at + BAND, :]
        pm[1, at:at + BAND, :] = y
        for k in range(0, BAND // local, 2):
            s = at // local + k
            theirs = split3_rows(
                jnp.concatenate([y[(k + j) * local:(k + j + 1) * local] for j in range(2)], axis=1)
            )
            ours = jnp.concatenate([ym[s], ym[s + 1]], axis=1)
            total += outer(jnp.where(g == 0, ours, theirs), jnp.where(g == 0, theirs, ours))

    def finish_late():
        for first in range(0, cap, 256):
            arrive(1, first)
            parts = parts_at(1, first)
            for at in range(0, rows_all, BAND):
                y = placed(posm[at:at + BAND, :], first, parts, BAND)
                pm[0, at:at + BAND, :] = y if first == 0 else pm[0, at:at + BAND, :] + y

    value = pack(folded(total, local))
    for t in range(stages):
        copies += spread_out(members, t, slots[t], s_send[t], s_recv[t], value)
        if t == 0:
            for ch in range(EARLY, chunks):
                x_copy(1, ch).start()
        gather_in(members, t, own_slots[t], o_send[t], o_recv[t])
        n = members[t][0]
        if t == 0:
            own_total = jnp.concatenate(
                [total_of(own_slots[0], 0, n // 2), total_of(own_slots[0], n // 2, n)], axis=0
            )
        else:
            own_total = total_of(own_slots[t], 0, n)
        if t + 1 < stages:
            copies += spread_out(members, t + 1, own_slots[t + 1], o_send[t + 1], o_recv[t + 1], own_total)
        else:
            finish_late()
        gather_in(members, t, slots[t], s_send[t], s_recv[t])
        value = total_of(slots[t], 0, members[t][0])

    upper = unpack(value, local)
    square = jnp.concatenate([upper, jnp.zeros((128 - local, 128), F32)], axis=0)
    lower = square.T[:local]
    value = jnp.concatenate(
        [
            unpack(own_total[:8], local) + pltpu.roll(upper, local, 1),
            lower + pltpu.roll(unpack(own_total[8:], local), local, 1),
        ],
        axis=0,
    )
    coef_wide, eye = solve(value, grids)
    coef_out[...] = jnp.sum(jnp.where(eye, coef_wide, 0.0), axis=0, keepdims=True)[:, :grids]

    ours = jnp.where(g == 0, coef_wide[:local], coef_wide[local:])
    theirs = jnp.where(g == 0, coef_wide[local:], coef_wide[:local])
    if half > 128:
        ours, theirs = [jnp.concatenate([w] * (half // 128), axis=1) for w in (ours, theirs)]
    for h, slot in ((0, other), (1, g)):
        for first in range(0, subs, 8):
            at = first * local
            acc = xm[h, first:first + 8] * ours[None] + (
                pm[h, at:at + 8 * local, :].reshape(8, local, half) * theirs[None]
            )
            cbuf[slot, first:first + 8] = jnp.sum(acc, axis=1)
    for h in range(groups):
        comb_out[:, h * half:(h + 1) * half] = cbuf[h]

    for copy in copies:
        copy.wait_send()
    lev_copy.wait_send()
    for h in range(2):
        for ch in range(chunks):
            x_copy(h, ch).wait_send()


def spread(combined, coef, lev, updated, coef_out, block, sems):
    local, subs, cells = updated.shape
    coef_out[...] = coef[...]
    dig0, dig1, dig2 = digits_of(lax.broadcasted_iota(jnp.int32, (subs, 128), 0))
    copies = []
    for i in range(local):
        keep = (lev[0, i:i + 1, :] >= dig0) & (lev[1, i:i + 1, :] >= dig1) & (lev[2, i:i + 1, :] >= dig2)
        for c in range(0, cells, 128):
            block[i, :, c:c + 128] = jnp.where(keep, combined[:, c:c + 128], 0.0)
        if (i + 1) % SPREAD == 0 or i + 1 == local:
            n = len(copies)
            part = pl.ds(n * SPREAD, i + 1 - n * SPREAD)
            copy = pltpu.make_async_copy(block.at[part], updated.at[part], sems.at[n])
            copy.start()
            copies.append(copy)
    for copy in copies:
        copy.wait()


def dense_call(groups, radices, surplus, levels, identity):
    local, subs, cells = surplus.shape
    grids = groups * local
    half = cells // groups
    sizes = [groups * r if t == 0 else r for t, r in enumerate(radices)]
    dma = pltpu.SemaphoreType.DMA
    chunks = subs // ROWS
    return pl.pallas_call(
        functools.partial(kernel, groups, radices, local, subs),
        out_shape=(
            jax.ShapeDtypeStruct((subs, cells), F32),
            jax.ShapeDtypeStruct((1, grids), F32),
            jax.ShapeDtypeStruct((3, local, 128), F32),
        ),
        in_specs=[pl.BlockSpec(memory_space=pltpu.HBM), pl.BlockSpec(memory_space=pltpu.VMEM)],
        out_specs=tuple(pl.BlockSpec(memory_space=pltpu.VMEM) for _ in range(3)),
        scratch_shapes=[
            pltpu.VMEM((grids, subs, half), F32),
            pltpu.VMEM((groups, 3, local), jnp.int32),
            pltpu.VMEM((3, grids, 128), F32),
            pltpu.VMEM((3 * grids, 3 * grids), F32),
            pltpu.VMEM((groups, subs, half), F32),
            dma(()), dma((groups,)), dma((groups,)),
            dma((groups, chunks)), dma((groups, chunks)), dma((groups, PIECES)), dma((groups, PIECES)),
        ]
        + [pltpu.VMEM((n, grids // 2, 128), F32) for n in sizes]
        + [dma((n,)) for n in sizes]
        + [dma((n,)) for n in sizes],
        compiler_params=pltpu.CompilerParams(
            collective_id=identity, has_side_effects=True, vmem_limit_bytes=VMEM_BYTES
        ),
    )(surplus, levels)


def sparse_call(groups, radices, surplus, levels, identity):
    local, subs, cells = surplus.shape
    grids = groups * local
    half = cells // groups
    cap = local * subs // 3 // 256 * 256
    chunks = cap // STEP
    sizes = [groups * r if t == 0 else r for t, r in enumerate(radices)]
    dma = pltpu.SemaphoreType.DMA
    return pl.pallas_call(
        functools.partial(sparse_kernel, groups, radices, local, subs, cap),
        out_shape=(
            jax.ShapeDtypeStruct((subs, cells), F32),
            jax.ShapeDtypeStruct((1, grids), F32),
            jax.ShapeDtypeStruct((3, local, 128), F32),
            jax.ShapeDtypeStruct((1, 1), jnp.int32),
        ),
        in_specs=[pl.BlockSpec(memory_space=pltpu.HBM), pl.BlockSpec(memory_space=pltpu.HBM)],
        out_specs=tuple(pl.BlockSpec(memory_space=pltpu.VMEM) for _ in range(3))
        + (pl.BlockSpec(memory_space=pltpu.SMEM),),
        scratch_shapes=[
            pltpu.VMEM((2, local, subs, half), F32),
            pltpu.VMEM((2, subs, local, half), F32),
            pltpu.VMEM((2, local * subs, 3 * half), jnp.bfloat16),
            pltpu.VMEM((subs, 3 * local, half), jnp.bfloat16),
            pltpu.VMEM((2, local * subs, half), F32),
            pltpu.VMEM((2, cap, half), F32),
            pltpu.VMEM((2, cap, half), F32),
            pltpu.VMEM((local * subs, 128), F32),
            pltpu.VMEM((groups, 3, local), jnp.int32),
            pltpu.VMEM((3 * local, 3 * local), F32),
            pltpu.VMEM((groups, subs, half), F32),
            dma((3,)), dma((2, local)), dma((2,)), dma((2, chunks)), dma((2, chunks)),
        ]
        + [pltpu.VMEM((n, 8, 128), F32) for n in sizes]
        + [dma((n,)) for n in sizes]
        + [dma((n,)) for n in sizes]
        + [pltpu.VMEM((n, 8 if t == 0 else 16, 128), F32) for t, n in enumerate(sizes)]
        + [dma((n,)) for n in sizes]
        + [dma((n,)) for n in sizes],
        compiler_params=pltpu.CompilerParams(
            collective_id=identity, has_side_effects=True, vmem_limit_bytes=VMEM_BYTES
        ),
    )(surplus, levels)


def shards(groups, domains, surplus, levels):
    local, subs, cells = surplus.shape
    grids = groups * local
    radices = radices_of(domains)
    flipped = levels.T
    *found, fits = sparse_call(groups, radices, surplus, flipped, 0)
    combined, coefficients, lev_wide = lax.cond(
        fits[0, 0] == 1,
        lambda *kept: tuple(kept[2:]),
        lambda *kept: tuple(dense_call(groups, radices, kept[0], kept[1], 1)),
        surplus, flipped, *found,
    )
    updated, coefficients = pl.pallas_call(
        spread,
        out_shape=(
            jax.ShapeDtypeStruct((local, subs, cells), F32),
            jax.ShapeDtypeStruct((1, grids), F32),
        ),
        in_specs=[pl.BlockSpec(memory_space=pltpu.VMEM)] * 3,
        out_specs=(pl.BlockSpec(memory_space=pl.ANY), pl.BlockSpec(memory_space=pltpu.VMEM)),
        scratch_shapes=[pltpu.VMEM((local, subs, cells), F32), pltpu.SemaphoreType.DMA((-(-local // SPREAD),))],
        compiler_params=pltpu.CompilerParams(vmem_limit_bytes=VMEM_BYTES),
    )(combined, coefficients, lev_wide)
    return (updated, coefficients.reshape(grids))


def solution(mesh):
    placed = (P("grp", None, "dom"), P("grp", None))
    return jax.shard_map(
        functools.partial(shards, mesh.shape["grp"], mesh.shape["dom"]),
        mesh=mesh, in_specs=placed, out_specs=(P("grp", None, "dom"), P()), check_vma=False,
    )
```

```python
import functools

import jax
import jax.numpy as jnp
from jax import lax
from jax.experimental import pallas as pl
from jax.experimental.pallas import tpu as pltpu
from jax.sharding import PartitionSpec as P

MESH = pl.DeviceIdType.MESH
ROWS = 8
BLOCK = 16
PIECES = 2
SPREAD = 4
SLOT = 32
STEP = 128
EARLY = 0
BAND = 384
VMEM_BYTES = 32 * 1024 * 1024
F32 = jnp.float32


def radices_of(size):
    out = []
    while size > 1:
        for r in (4, 2, 3, 5, 7, size):
            if size % r == 0:
                out.append(r)
                size //= r
                break
    return out


def digits_of(sub):
    return (sub // 16).astype(F32), lax.rem(sub // 4, 4).astype(F32), lax.rem(sub, 4).astype(F32)


def split3(x):
    hi = x.astype(jnp.bfloat16)
    rest = x - hi.astype(F32)
    mid = rest.astype(jnp.bfloat16)
    lo = (rest - mid.astype(F32)).astype(jnp.bfloat16)
    return jnp.concatenate([hi, mid, lo], axis=0)


def kernel(groups, radices, local, subs, surplus, levels, comb_out, coef_out, lev_out, *scratch):
    stages = len(radices)
    (xb, lev, lbc, prod, cbuf, local_sem, lev_send, lev_recv, x_send, x_recv, c_send, c_recv) = scratch[:12]
    slots = scratch[12:12 + stages]
    s_send = scratch[12 + stages:12 + 2 * stages]
    s_recv = scratch[12 + 2 * stages:12 + 3 * stages]
    grids = groups * local
    half = xb.shape[-1]
    chunks = subs // ROWS
    g = lax.axis_index("grp")
    d = lax.axis_index("dom")

    members = []
    stride = 1
    for t, r in enumerate(radices):
        digit = lax.rem(d // stride, r)
        base = d - digit * stride
        if t == 0:
            n = groups * r
            mine = g * r + digit
            device = functools.partial(lambda b, r_, q: (q // r_, b + lax.rem(q, r_)), base, r)
        else:
            n = r
            mine = digit
            device = functools.partial(lambda b, st, q: (g, b + q * st), base, stride)
        members.append((n, mine, device))
        stride *= r

    barrier = pltpu.get_barrier_semaphore()
    count = 0
    for n, mine, device in members:
        for k in range(1, n):
            q = lax.rem(mine + k, n)
            pl.semaphore_signal(barrier, inc=1, device_id=device(q), device_id_type=MESH)
            count += 1

    own_cells = pl.ds(pl.multiple_of(g * half, half), half)
    own_copy = pltpu.make_async_copy(
        surplus.at[:, :, own_cells], xb.at[pl.ds(g * local, local)], local_sem
    )
    own_copy.start()
    pl.semaphore_wait(barrier, count)

    def lev_copy(k):
        q = lax.rem(g + k, groups)
        return pltpu.make_async_remote_copy(
            src_ref=levels, dst_ref=lev.at[g], send_sem=lev_send.at[k], recv_sem=lev_recv.at[g],
            device_id=(q, d), device_id_type=MESH,
        )

    def x_copy(k, ch):
        q = lax.rem(g + k, groups)
        rows = pl.ds(pl.multiple_of(ch * ROWS, ROWS), ROWS)
        return pltpu.make_async_remote_copy(
            src_ref=surplus.at[:, rows, pl.ds(pl.multiple_of(q * half, half), half)],
            dst_ref=xb.at[pl.ds(g * local, local), rows],
            send_sem=x_send.at[k, ch], recv_sem=x_recv.at[g, ch],
            device_id=(q, d), device_id_type=MESH,
        )

    def x_arrival(k, ch):
        q = lax.rem(g + k, groups)
        rows = pl.ds(pl.multiple_of(ch * ROWS, ROWS), ROWS)
        block = xb.at[pl.ds(q * local, local), rows]
        return pltpu.make_async_remote_copy(
            src_ref=block, dst_ref=block, send_sem=x_send.at[k, ch], recv_sem=x_recv.at[q, ch],
            device_id=(q, d), device_id_type=MESH,
        )

    for k in range(1, groups):
        lev_copy(k).start()
    for ch in range(chunks):
        for k in range(1, groups):
            x_copy(k, ch).start()

    lev[g] = levels[...]
    for k in range(1, groups):
        q = lax.rem(g + k, groups)
        pltpu.make_async_remote_copy(
            src_ref=lev.at[q], dst_ref=lev.at[q], send_sem=lev_send.at[k], recv_sem=lev_recv.at[q],
            device_id=(q, d), device_id_type=MESH,
        ).wait_recv()
    lev_eye = lax.broadcasted_iota(jnp.int32, (local, local), 0) == lax.broadcasted_iota(
        jnp.int32, (local, local), 1
    )
    for h in range(groups):
        for axis in range(3):
            lev_row = lev[h, axis:axis + 1, :].astype(F32)
            lev_col = jnp.sum(jnp.where(lev_eye, lev_row, 0.0), axis=1, keepdims=True)
            lbc[axis, pl.ds(h * local, local), :] = jnp.broadcast_to(lev_col, (local, 128))
    lev_out[...] = lbc[:, pl.ds(pl.multiple_of(g * local, 8), local), :]
    prod[...] = jnp.zeros_like(prod)
    own_copy.wait()
    flat = xb.reshape(grids * subs, half)

    def gram_chunk(ch, carry):
        for k in range(1, groups):
            x_arrival(k, ch).wait_recv()
        lev0, lev1, lev2 = lbc[0], lbc[1], lbc[2]
        total = jnp.zeros(prod.shape, F32)
        for pair in range(0, ROWS, 2):
            parts = []
            for k in range(pair, pair + 2):
                s = ch * ROWS + k
                x = flat[pl.ds(s, grids, stride=subs), :]
                keep = (
                    (lev0 >= (s // 16).astype(F32))
                    & (lev1 >= lax.rem(s // 4, 4).astype(F32))
                    & (lev2 >= float(k % 4))
                )
                keep = jnp.concatenate([keep] * (half // 128), axis=1) if half > 128 else keep
                parts.append(jnp.where(keep, x, 0.0))
            y = split3(jnp.concatenate(parts, axis=1))
            total += lax.dot_general(y, y, (((1,), (1,)), ((), ())), preferred_element_type=F32)
        prod[...] += total
        return carry

    lax.fori_loop(0, chunks, gram_chunk, 0)

    part = prod[2 * grids:, :] + prod[grids:2 * grids, :] + prod[:grids, :]
    part = part[:, 2 * grids:] + part[:, grids:2 * grids] + part[:, :grids]
    value = jnp.concatenate([part, jnp.zeros((grids, 128 - grids), F32)], axis=1)
    fold = grids // 2
    value = value[:fold] + pltpu.roll(value[fold:], 64, 1)

    copies = []
    for t, (n, mine, device) in enumerate(members):
        buf, send, recv = slots[t], s_send[t], s_recv[t]
        buf[mine] = value
        for k in range(1, n):
            q = lax.rem(mine + k, n)
            copy = pltpu.make_async_remote_copy(
                src_ref=buf.at[mine], dst_ref=buf.at[mine], send_sem=send.at[k], recv_sem=recv.at[mine],
                device_id=device(q), device_id_type=MESH,
            )
            copy.start()
            copies.append(copy)
        for k in range(1, n):
            q = lax.rem(mine + k, n)
            pltpu.make_async_remote_copy(
                src_ref=buf.at[q], dst_ref=buf.at[q], send_sem=send.at[k], recv_sem=recv.at[q],
                device_id=device(q), device_id_type=MESH,
            ).wait_recv()
        value = buf[0]
        for q in range(1, n):
            value = value + buf[q]

    left = lax.broadcasted_iota(jnp.int32, (fold, 128), 1) < 64
    value = jnp.concatenate(
        [jnp.where(left, value, 0.0), jnp.where(left, pltpu.roll(value, 64, 1), 0.0)], axis=0
    )

    row = lax.broadcasted_iota(jnp.int32, (grids, 128), 0)
    col = lax.broadcasted_iota(jnp.int32, (grids, 128), 1)
    eye = row == col
    diag = jnp.where(eye, value, 0.0)
    diag_col = jnp.sum(diag, axis=1, keepdims=True) + 1e-06
    diag_row = jnp.sum(diag, axis=0, keepdims=True) + 1e-06
    scale_col = 1.0 / jnp.sqrt(diag_col)
    scale_row = 1.0 / jnp.sqrt(diag_row)
    system = scale_col * value * scale_row + jnp.where(eye, 0.1, 0.0)
    system = jnp.where(col == grids, jnp.sqrt(diag_col), jnp.where(col < grids, system, 0.0))
    for first in range(0, grids, BLOCK):
        width = min(BLOCK, grids - first)
        rows = [system[first + j:first + j + 1, :] for j in range(width)]
        cols = [
            jnp.broadcast_to(system[:, first + j:first + j + 1], (grids, 128)) for j in range(width)
        ]
        for j in range(width):
            k = first + j
            inverse = 1.0 / cols[j][k:k + 1, :]
            factor = jnp.where(row == k, 0.0, cols[j] * inverse)
            for m in range(j + 1, width):
                cols[m] = cols[m] - factor * cols[m][k:k + 1, :]
                rows[m] = rows[m] - factor[first + m:first + m + 1, :] * rows[j]
            system = system - factor * rows[j]
    final = jnp.sum(jnp.where(eye, system, 0.0), axis=1, keepdims=True)
    coef = scale_col * (system[:, grids:grids + 1] / final)
    coef_wide = jnp.broadcast_to(coef, (grids, 128))
    coef_out[...] = jnp.sum(jnp.where(eye, coef_wide, 0.0), axis=0, keepdims=True)[:, :grids]

    piece = subs // PIECES

    def c_copy(slot, k, p):
        block = cbuf.at[slot, pl.ds(p * piece, piece)]
        return pltpu.make_async_remote_copy(
            src_ref=block, dst_ref=block, send_sem=c_send.at[k, p], recv_sem=c_recv.at[slot, p],
            device_id=(lax.rem(g + k, groups), d), device_id_type=MESH,
        )

    for p in range(PIECES):
        sub = lax.broadcasted_iota(jnp.int32, (piece, half), 0) + p * piece
        dig0, dig1, dig2 = digits_of(sub)
        acc = jnp.zeros((piece, half), F32)
        for i in range(grids):
            keep = (
                (lbc[0, i:i + 1, 0:1] >= dig0)
                & (lbc[1, i:i + 1, 0:1] >= dig1)
                & (lbc[2, i:i + 1, 0:1] >= dig2)
            )
            acc += jnp.where(keep, coef_wide[i:i + 1, 0:1], 0.0) * xb[i, p * piece:(p + 1) * piece]
        cbuf[g, p * piece:(p + 1) * piece] = acc
        for k in range(1, groups):
            c_copy(g, k, p).start()
    for p in range(PIECES):
        for k in range(1, groups):
            c_copy(lax.rem(g + k, groups), k, p).wait_recv()
    for h in range(groups):
        comb_out[:, h * half:(h + 1) * half] = cbuf[h]

    for copy in copies:
        copy.wait_send()
    for k in range(1, groups):
        lev_copy(k).wait_send()
        for ch in range(chunks):
            x_copy(k, ch).wait_send()
        for p in range(PIECES):
            c_copy(g, k, p).wait_send()


def split3_rows(x):
    hi = x.astype(jnp.bfloat16).astype(F32)
    rest = x - hi
    mid = rest.astype(jnp.bfloat16).astype(F32)
    return jnp.concatenate([hi, mid, rest - mid], axis=0).astype(jnp.bfloat16)


def layout_of(groups, radices, g, d):
    members = []
    stride = 1
    for t, r in enumerate(radices):
        digit = lax.rem(d // stride, r)
        base = d - digit * stride
        if t == 0:
            n = groups * r
            mine = g * r + digit
            device = functools.partial(lambda b, r_, q: (q // r_, b + lax.rem(q, r_)), base, r)
        else:
            n = r
            mine = digit
            device = functools.partial(lambda b, st, q: (g, b + q * st), base, stride)
        members.append((n, mine, device))
        stride *= r
    return members


def spread_out(members, t, buf, send, recv, value):
    n, mine, device = members[t]
    buf[mine] = value
    copies = []
    for k in range(1, n):
        copy = pltpu.make_async_remote_copy(
            src_ref=buf.at[mine], dst_ref=buf.at[mine], send_sem=send.at[k], recv_sem=recv.at[mine],
            device_id=device(lax.rem(mine + k, n)), device_id_type=MESH,
        )
        copy.start()
        copies.append(copy)
    return copies


def gather_in(members, t, buf, send, recv):
    n, mine, device = members[t]
    for k in range(1, n):
        q = lax.rem(mine + k, n)
        pltpu.make_async_remote_copy(
            src_ref=buf.at[q], dst_ref=buf.at[q], send_sem=send.at[k], recv_sem=recv.at[q],
            device_id=device(q), device_id_type=MESH,
        ).wait_recv()


def total_of(buf, first, last):
    value = buf[first]
    for q in range(first + 1, last):
        value = value + buf[q]
    return value


def pack(square):
    local = square.shape[0]
    wide = jnp.concatenate([square, jnp.zeros((local, 128 - local), F32)], axis=1)
    out = wide[:8]
    for b in range(1, local // 8):
        out = out + pltpu.roll(wide[8 * b:8 * b + 8], SLOT * b, 1)
    return out


def unpack(packed, local):
    rows = [packed] + [pltpu.roll(packed, 128 - SLOT * b, 1) for b in range(1, local // 8)]
    wide = jnp.concatenate(rows, axis=0)
    return jnp.where(lax.broadcasted_iota(jnp.int32, (local, 128), 1) < local, wide, 0.0)


def folded(products, n):
    part = products[2 * n:, :] + products[n:2 * n, :] + products[:n, :]
    return part[:, 2 * n:] + part[:, n:2 * n] + part[:, :n]


def outer(a, b):
    return lax.dot_general(a, b, (((1,), (1,)), ((), ())), preferred_element_type=F32)


def count_dot(a, b):
    bf16 = jnp.bfloat16
    return jnp.dot(a.astype(bf16), b.astype(bf16), preferred_element_type=F32)


def below(n, m, flip):
    r = lax.broadcasted_iota(jnp.int32, (n, m), 0)
    c = lax.broadcasted_iota(jnp.int32, (n, m), 1)
    return jnp.where((r < c) if flip else (r > c), 1.0, 0.0)


def solve(value, grids):
    row = lax.broadcasted_iota(jnp.int32, (grids, 128), 0)
    col = lax.broadcasted_iota(jnp.int32, (grids, 128), 1)
    eye = row == col
    diag = jnp.where(eye, value, 0.0)
    diag_col = jnp.sum(diag, axis=1, keepdims=True) + 1e-06
    diag_row = jnp.sum(diag, axis=0, keepdims=True) + 1e-06
    scale_col = 1.0 / jnp.sqrt(diag_col)
    scale_row = 1.0 / jnp.sqrt(diag_row)
    system = scale_col * value * scale_row + jnp.where(eye, 0.1, 0.0)
    system = jnp.where(col == grids, jnp.sqrt(diag_col), jnp.where(col < grids, system, 0.0))
    for first in range(0, grids, BLOCK):
        width = min(BLOCK, grids - first)
        rows = [system[first + j:first + j + 1, :] for j in range(width)]
        cols = [
            jnp.broadcast_to(system[:, first + j:first + j + 1], (grids, 128)) for j in range(width)
        ]
        for j in range(width):
            k = first + j
            inverse = 1.0 / cols[j][k:k + 1, :]
            factor = jnp.where(row == k, 0.0, cols[j] * inverse)
            for m in range(j + 1, width):
                cols[m] = cols[m] - factor * cols[m][k:k + 1, :]
                rows[m] = rows[m] - factor[first + m:first + m + 1, :] * rows[j]
            system = system - factor * rows[j]
    final = jnp.sum(jnp.where(eye, system, 0.0), axis=1, keepdims=True)
    coef = scale_col * (system[:, grids:grids + 1] / final)
    return jnp.broadcast_to(coef, (grids, 128)), eye


def parts_of(x):
    hi = x.astype(jnp.bfloat16)
    left = x - hi.astype(F32)
    mid = left.astype(jnp.bfloat16)
    return hi, mid, (left - mid.astype(F32)).astype(jnp.bfloat16)


def places_of(keep, across):
    n, m = keep.shape
    if across:
        totals = count_dot(jnp.ones((n, n), F32), keep)
        pos = count_dot(below(n, n, False), keep) + count_dot(totals, below(m, m, True))
    else:
        totals = count_dot(keep, jnp.ones((m, m), F32))
        pos = count_dot(below(n, n, False), totals) + count_dot(keep, below(m, m, True))
    return jnp.where(keep > 0.0, pos, -1.0)


def sparse_kernel(groups, radices, local, subs, cap, surplus, levels, comb_out, coef_out, lev_out, fits_out, *scratch):
    stages = len(radices)
    (xh, xm, xs, ym, pm, csend, crecv, posm, lev, prod, local_sem, m_sem, lev_sem, x_send,
     x_recv) = scratch[:15]
    rest = [scratch[15 + m * stages:15 + (m + 1) * stages] for m in range(6)]
    slots, s_send, s_recv, own_slots, o_send, o_recv = rest
    grids = groups * local
    half = xh.shape[-1]
    rows_all = local * subs
    chunks = cap // STEP
    bf16 = jnp.bfloat16
    g = lax.axis_index("grp")
    d = lax.axis_index("dom")
    other = 1 - g
    members = layout_of(groups, radices, g, d)

    cells = [pl.ds(pl.multiple_of(h * half, half), half) for h in (other, g)]
    lev_load = pltpu.make_async_copy(levels, lev.at[g], local_sem.at[2])
    lev_load.start()
    loads = [pltpu.make_async_copy(surplus.at[:, :, cells[h]], xh.at[h], local_sem.at[h]) for h in range(2)]
    for load in loads:
        load.start()
    turns = [pltpu.make_async_copy(surplus.at[i], xm.at[:, i, :], m_sem.at[i]) for i in range(local)]

    barrier = pltpu.get_barrier_semaphore()
    count = 0
    for n, mine, device in members:
        for k in range(1, n):
            pl.semaphore_signal(barrier, inc=1, device_id=device(lax.rem(mine + k, n)), device_id_type=MESH)
            count += 1

    def lev_wide(h):
        eye = lax.broadcasted_iota(jnp.int32, (local, local), 0) == lax.broadcasted_iota(jnp.int32, (local, local), 1)
        out = []
        for axis in range(3):
            lev_row = lev[h, axis:axis + 1, :].astype(F32)
            lev_col = jnp.sum(jnp.where(eye, lev_row, 0.0), axis=1, keepdims=True)
            out.append(jnp.broadcast_to(lev_col, (local, 128)))
        return out

    def kept_by(wide):
        digits = digits_of(lax.broadcasted_iota(jnp.int32, (local, 128), 1))
        keep = jnp.ones((local, 128), F32)
        for axis in range(3):
            keep = jnp.where(wide[axis] >= digits[axis], keep, 0.0)
        return keep

    lev_load.wait()
    wide = lev_wide(g)
    for axis in range(3):
        lev_out[axis] = wide[axis]
    keep = kept_by(wide)
    own_count = jnp.sum(keep)
    pos = places_of(keep, True)
    pos_far = pltpu.roll(pos, 64, 1)
    low = lax.broadcasted_iota(jnp.int32, (1, 128), 1) < subs
    pos_rows = [jnp.where(low, pos[i:i + 1], pos_far[i + 1:i + 2]) for i in range(0, local, 128 // subs)]

    def split_half(h):
        flat = xh.at[h].reshape(rows_all, half)
        for i in range(0, rows_all, 256):
            for m, part in enumerate(parts_of(flat[i:i + 256, :])):
                xs[h, i:i + 256, m * half:(m + 1) * half] = part

    loads[0].wait()
    for turn in turns:
        turn.start()
    split_half(0)
    def x_copy(h, ch):
        rows = pl.ds(pl.multiple_of(ch * STEP, STEP), STEP)
        return pltpu.make_async_remote_copy(
            src_ref=csend.at[h, rows], dst_ref=crecv.at[h, rows], send_sem=x_send.at[h, ch], recv_sem=x_recv.at[h, ch],
            device_id=(other, d), device_id_type=MESH,
        )

    index = lax.broadcasted_iota(jnp.int32, (256, 128), 0).astype(F32)

    def gather_rows(h, first):
        want = index + float(first)
        acc = jnp.zeros((256, 3 * half), F32)
        for m in range(0, len(pos_rows), 2):
            picks = [jnp.where(want == p, 1.0, 0.0).astype(bf16) for p in pos_rows[m:m + 2]]
            acc += jnp.dot(
                jnp.concatenate(picks, axis=1), xs[h, m * 128:m * 128 + 256, :], preferred_element_type=F32
            )
        csend[h, first:first + 256, :] = acc[:, :half] + acc[:, half:2 * half] + acc[:, 2 * half:]

    def depart(h, first, last):
        for ch in range(first // STEP, last // STEP):
            x_copy(h, ch).start()

    gather_rows(0, 0)
    pl.semaphore_wait(barrier, count)
    lev_copy = pltpu.make_async_remote_copy(
        src_ref=lev.at[g], dst_ref=lev.at[g], send_sem=lev_sem.at[0], recv_sem=lev_sem.at[1],
        device_id=(other, d), device_id_type=MESH,
    )
    lev_copy.start()
    depart(0, 0, 256)
    for first in range(256, cap, 256):
        gather_rows(0, first)
        depart(0, first, first + 256)
    loads[1].wait()
    split_half(1)
    gather_rows(1, 0)
    depart(1, 0, EARLY)

    for turn in turns:
        turn.wait()
    prod[...] = jnp.zeros_like(prod)

    def own_gram(ch, carry):
        total = jnp.zeros(prod.shape, F32)
        for k in range(ROWS):
            s = ch * ROWS + k
            own = (
                (lev_out[0] >= (s // 16).astype(F32))
                & (lev_out[1] >= lax.rem(s // 4, 4).astype(F32))
                & (lev_out[2] >= float(k % 4))
            )
            own = jnp.concatenate([own] * (groups * half // 128), axis=1)
            x = jnp.where(own, xm[s], 0.0)
            xm[s] = x
            y = split3_rows(x)
            ym[s] = jnp.where(g == 0, y[:, :half], y[:, half:])
            total += outer(y, y)
        prod[...] += total
        return carry

    lax.fori_loop(0, subs // ROWS, own_gram, 0)

    lev_copy.wait_recv()
    keep = kept_by(lev_wide(other))
    fits_out[0, 0] = jnp.where(jnp.maximum(own_count, jnp.sum(keep)) <= float(cap), 1, 0)
    pos = places_of(keep, True)
    for s in range(subs):
        posm[s * local:(s + 1) * local, :] = jnp.broadcast_to(pos[:, s:s + 1], (local, 128))

    copies = spread_out(members, 0, own_slots[0], o_send[0], o_recv[0], pack(folded(prod[...], local)))

    def parts_at(h, first):
        return jnp.concatenate(parts_of(crecv[h, first:first + 256, :]), axis=1)

    def placed(where, first, parts, n):
        lane = lax.broadcasted_iota(jnp.int32, (n, 128), 1).astype(F32) + float(first)
        picks = [jnp.where(where == lane + float(c), 1.0, 0.0).astype(bf16) for c in range(0, 256, 128)]
        y = jnp.dot(jnp.concatenate(picks, axis=1), parts, preferred_element_type=F32)
        return y[:, :half] + y[:, half:2 * half] + y[:, 2 * half:]

    def arrive(h, first):
        for ch in range(first // STEP, (first + 256) // STEP):
            x_copy(h, ch).wait_recv()

    last = cap - 256
    for first in range(0, last, 256):
        arrive(0, first)
        parts = parts_at(0, first)

        for at in range(0, rows_all, BAND):
            y = placed(posm[at:at + BAND, :], first, parts, BAND)
            pm[g, at:at + BAND, :] = y if first == 0 else pm[g, at:at + BAND, :] + y

    arrive(0, last)
    parts = parts_at(0, last)
    total = jnp.zeros((3 * local, 3 * local), F32)
    for at in range(0, rows_all, BAND):
        y = placed(posm[at:at + BAND, :], last, parts, BAND)
        if last > 0:
            y = y + pm[g, at:at + BAND, :]
        pm[g, at:at + BAND, :] = y
        for k in range(0, BAND // local, 2):
            s = at // local + k
            theirs = split3_rows(
                jnp.concatenate([y[(k + j) * local:(k + j + 1) * local] for j in range(2)], axis=1)
            )
            ours = jnp.concatenate([ym[s], ym[s + 1]], axis=1)
            total += outer(jnp.where(g == 0, ours, theirs), jnp.where(g == 0, theirs, ours))

    def finish_late():
        for first in range(0, cap, 256):
            arrive(1, first)
            parts = parts_at(1, first)
            for at in range(0, rows_all, BAND):
                y = placed(posm[at:at + BAND, :], first, parts, BAND)
                pm[other, at:at + BAND, :] = y if first == 0 else pm[other, at:at + BAND, :] + y

    value = pack(folded(total, local))
    for t in range(stages):
        copies += spread_out(members, t, slots[t], s_send[t], s_recv[t], value)
        if t == 0:
            depart(1, EARLY, 256)
            for first in range(256, cap, 256):
                gather_rows(1, first)
                depart(1, first, first + 256)
        gather_in(members, t, own_slots[t], o_send[t], o_recv[t])
        n = members[t][0]
        if t == 0:
            own_total = jnp.concatenate(
                [total_of(own_slots[0], 0, n // 2), total_of(own_slots[0], n // 2, n)], axis=0
            )
        else:
            own_total = total_of(own_slots[t], 0, n)
        if t + 1 < stages:
            copies += spread_out(members, t + 1, own_slots[t + 1], o_send[t + 1], o_recv[t + 1], own_total)
        else:
            finish_late()
        gather_in(members, t, slots[t], s_send[t], s_recv[t])
        value = total_of(slots[t], 0, members[t][0])

    upper = unpack(value, local)
    square = jnp.concatenate([upper, jnp.zeros((128 - local, 128), F32)], axis=0)
    lower = square.T[:local]
    value = jnp.concatenate(
        [
            unpack(own_total[:8], local) + pltpu.roll(upper, local, 1),
            lower + pltpu.roll(unpack(own_total[8:], local), local, 1),
        ],
        axis=0,
    )
    coef_wide, eye = solve(value, grids)
    coef_out[...] = jnp.sum(jnp.where(eye, coef_wide, 0.0), axis=0, keepdims=True)[:, :grids]

    ours = jnp.where(g == 0, coef_wide[:local], coef_wide[local:])
    theirs = jnp.where(g == 0, coef_wide[local:], coef_wide[:local])
    if half > 128:
        ours, theirs = [jnp.concatenate([w] * (half // 128), axis=1) for w in (ours, theirs)]
    for h in range(groups):
        for first in range(0, subs, 8):
            at = first * local
            acc = xm[first:first + 8, :, h * half:(h + 1) * half] * ours[None] + (
                pm[h, at:at + 8 * local, :].reshape(8, local, half) * theirs[None]
            )
            comb_out[first:first + 8, h * half:(h + 1) * half] = jnp.sum(acc, axis=1)

    for copy in copies:
        copy.wait_send()
    lev_copy.wait_send()
    for h in range(2):
        for ch in range(chunks):
            x_copy(h, ch).wait_send()


def spread(combined, coef, lev, updated, coef_out, block, sems):
    local, subs, cells = updated.shape
    coef_out[...] = coef[...]
    dig0, dig1, dig2 = digits_of(lax.broadcasted_iota(jnp.int32, (subs, 128), 0))
    copies = []
    for i in range(local):
        keep = (lev[0, i:i + 1, :] >= dig0) & (lev[1, i:i + 1, :] >= dig1) & (lev[2, i:i + 1, :] >= dig2)
        for c in range(0, cells, 128):
            block[i, :, c:c + 128] = jnp.where(keep, combined[:, c:c + 128], 0.0)
        if (i + 1) % SPREAD == 0 or i + 1 == local:
            n = len(copies)
            part = pl.ds(n * SPREAD, i + 1 - n * SPREAD)
            copy = pltpu.make_async_copy(block.at[part], updated.at[part], sems.at[n])
            copy.start()
            copies.append(copy)
    for copy in copies:
        copy.wait()


def dense_call(groups, radices, surplus, levels, identity):
    local, subs, cells = surplus.shape
    grids = groups * local
    half = cells // groups
    sizes = [groups * r if t == 0 else r for t, r in enumerate(radices)]
    dma = pltpu.SemaphoreType.DMA
    chunks = subs // ROWS
    return pl.pallas_call(
        functools.partial(kernel, groups, radices, local, subs),
        out_shape=(
            jax.ShapeDtypeStruct((subs, cells), F32),
            jax.ShapeDtypeStruct((1, grids), F32),
            jax.ShapeDtypeStruct((3, local, 128), F32),
        ),
        in_specs=[pl.BlockSpec(memory_space=pltpu.HBM), pl.BlockSpec(memory_space=pltpu.VMEM)],
        out_specs=tuple(pl.BlockSpec(memory_space=pltpu.VMEM) for _ in range(3)),
        scratch_shapes=[
            pltpu.VMEM((grids, subs, half), F32),
            pltpu.VMEM((groups, 3, local), jnp.int32),
            pltpu.VMEM((3, grids, 128), F32),
            pltpu.VMEM((3 * grids, 3 * grids), F32),
            pltpu.VMEM((groups, subs, half), F32),
            dma(()), dma((groups,)), dma((groups,)),
            dma((groups, chunks)), dma((groups, chunks)), dma((groups, PIECES)), dma((groups, PIECES)),
        ]
        + [pltpu.VMEM((n, grids // 2, 128), F32) for n in sizes]
        + [dma((n,)) for n in sizes]
        + [dma((n,)) for n in sizes],
        compiler_params=pltpu.CompilerParams(
            collective_id=identity, has_side_effects=True, vmem_limit_bytes=VMEM_BYTES
        ),
    )(surplus, levels)


def sparse_call(groups, radices, surplus, levels, identity):
    local, subs, cells = surplus.shape
    grids = groups * local
    half = cells // groups
    cap = local * subs // 3 // 256 * 256
    chunks = cap // STEP
    sizes = [groups * r if t == 0 else r for t, r in enumerate(radices)]
    dma = pltpu.SemaphoreType.DMA
    return pl.pallas_call(
        functools.partial(sparse_kernel, groups, radices, local, subs, cap),
        out_shape=(
            jax.ShapeDtypeStruct((subs, cells), F32),
            jax.ShapeDtypeStruct((1, grids), F32),
            jax.ShapeDtypeStruct((3, local, 128), F32),
            jax.ShapeDtypeStruct((1, 1), jnp.int32),
        ),
        in_specs=[pl.BlockSpec(memory_space=pltpu.HBM), pl.BlockSpec(memory_space=pltpu.HBM)],
        out_specs=tuple(pl.BlockSpec(memory_space=pltpu.VMEM) for _ in range(3))
        + (pl.BlockSpec(memory_space=pltpu.SMEM),),
        scratch_shapes=[
            pltpu.VMEM((2, local, subs, half), F32),
            pltpu.VMEM((subs, local, cells), F32),
            pltpu.VMEM((2, local * subs, 3 * half), jnp.bfloat16),
            pltpu.VMEM((subs, 3 * local, half), jnp.bfloat16),
            pltpu.VMEM((2, local * subs, half), F32),
            pltpu.VMEM((2, cap, half), F32),
            pltpu.VMEM((2, cap, half), F32),
            pltpu.VMEM((local * subs, 128), F32),
            pltpu.VMEM((groups, 3, local), jnp.int32),
            pltpu.VMEM((3 * local, 3 * local), F32),
            dma((3,)), dma((local,)), dma((2,)), dma((2, chunks)), dma((2, chunks)),
        ]
        + [pltpu.VMEM((n, 8, 128), F32) for n in sizes]
        + [dma((n,)) for n in sizes]
        + [dma((n,)) for n in sizes]
        + [pltpu.VMEM((n, 8 if t == 0 else 16, 128), F32) for t, n in enumerate(sizes)]
        + [dma((n,)) for n in sizes]
        + [dma((n,)) for n in sizes],
        compiler_params=pltpu.CompilerParams(
            collective_id=identity, has_side_effects=True, vmem_limit_bytes=VMEM_BYTES
        ),
    )(surplus, levels)


def shards(groups, domains, surplus, levels):
    local, subs, cells = surplus.shape
    grids = groups * local
    radices = radices_of(domains)
    flipped = levels.T
    *found, fits = sparse_call(groups, radices, surplus, flipped, 0)
    combined, coefficients, lev_wide = lax.cond(
        fits[0, 0] == 1,
        lambda *kept: tuple(kept[2:]),
        lambda *kept: tuple(dense_call(groups, radices, kept[0], kept[1], 1)),
        surplus, flipped, *found,
    )
    updated, coefficients = pl.pallas_call(
        spread,
        out_shape=(
            jax.ShapeDtypeStruct((local, subs, cells), F32),
            jax.ShapeDtypeStruct((1, grids), F32),
        ),
        in_specs=[pl.BlockSpec(memory_space=pltpu.VMEM)] * 3,
        out_specs=(pl.BlockSpec(memory_space=pl.ANY), pl.BlockSpec(memory_space=pltpu.VMEM)),
        scratch_shapes=[pltpu.VMEM((local, subs, cells), F32), pltpu.SemaphoreType.DMA((-(-local // SPREAD),))],
        compiler_params=pltpu.CompilerParams(vmem_limit_bytes=VMEM_BYTES),
    )(combined, coefficients, lev_wide)
    return (updated, coefficients.reshape(grids))


def solution(mesh):
    placed = (P("grp", None, "dom"), P("grp", None))
    return jax.shard_map(
        functools.partial(shards, mesh.shape["grp"], mesh.shape["dom"]),
        mesh=mesh, in_specs=placed, out_specs=(P("grp", None, "dom"), P()), check_vma=False,
    )
```

```python
import functools

import jax
import jax.numpy as jnp
from jax import lax
from jax.experimental import pallas as pl
from jax.experimental.pallas import tpu as pltpu
from jax.sharding import PartitionSpec as P

MESH = pl.DeviceIdType.MESH
ROWS = 8
BLOCK = 16
PIECES = 2
SPREAD = 4
SLOT = 32
STEP = 128
EARLY = 0
BAND = 384
VMEM_BYTES = 32 * 1024 * 1024
F32 = jnp.float32


def radices_of(size):
    out = []
    while size > 1:
        for r in (4, 2, 3, 5, 7, size):
            if size % r == 0:
                out.append(r)
                size //= r
                break
    return out


def digits_of(sub):
    return (sub // 16).astype(F32), lax.rem(sub // 4, 4).astype(F32), lax.rem(sub, 4).astype(F32)


def split3(x):
    hi = x.astype(jnp.bfloat16)
    rest = x - hi.astype(F32)
    mid = rest.astype(jnp.bfloat16)
    lo = (rest - mid.astype(F32)).astype(jnp.bfloat16)
    return jnp.concatenate([hi, mid, lo], axis=0)


def kernel(groups, radices, local, subs, surplus, levels, comb_out, coef_out, lev_out, *scratch):
    stages = len(radices)
    (xb, lev, lbc, prod, cbuf, local_sem, lev_send, lev_recv, x_send, x_recv, c_send, c_recv) = scratch[:12]
    slots = scratch[12:12 + stages]
    s_send = scratch[12 + stages:12 + 2 * stages]
    s_recv = scratch[12 + 2 * stages:12 + 3 * stages]
    grids = groups * local
    half = xb.shape[-1]
    chunks = subs // ROWS
    g = lax.axis_index("grp")
    d = lax.axis_index("dom")

    members = []
    stride = 1
    for t, r in enumerate(radices):
        digit = lax.rem(d // stride, r)
        base = d - digit * stride
        if t == 0:
            n = groups * r
            mine = g * r + digit
            device = functools.partial(lambda b, r_, q: (q // r_, b + lax.rem(q, r_)), base, r)
        else:
            n = r
            mine = digit
            device = functools.partial(lambda b, st, q: (g, b + q * st), base, stride)
        members.append((n, mine, device))
        stride *= r

    barrier = pltpu.get_barrier_semaphore()
    count = 0
    for n, mine, device in members:
        for k in range(1, n):
            q = lax.rem(mine + k, n)
            pl.semaphore_signal(barrier, inc=1, device_id=device(q), device_id_type=MESH)
            count += 1

    own_cells = pl.ds(pl.multiple_of(g * half, half), half)
    own_copy = pltpu.make_async_copy(
        surplus.at[:, :, own_cells], xb.at[pl.ds(g * local, local)], local_sem
    )
    own_copy.start()
    pl.semaphore_wait(barrier, count)

    def lev_copy(k):
        q = lax.rem(g + k, groups)
        return pltpu.make_async_remote_copy(
            src_ref=levels, dst_ref=lev.at[g], send_sem=lev_send.at[k], recv_sem=lev_recv.at[g],
            device_id=(q, d), device_id_type=MESH,
        )

    def x_copy(k, ch):
        q = lax.rem(g + k, groups)
        rows = pl.ds(pl.multiple_of(ch * ROWS, ROWS), ROWS)
        return pltpu.make_async_remote_copy(
            src_ref=surplus.at[:, rows, pl.ds(pl.multiple_of(q * half, half), half)],
            dst_ref=xb.at[pl.ds(g * local, local), rows],
            send_sem=x_send.at[k, ch], recv_sem=x_recv.at[g, ch],
            device_id=(q, d), device_id_type=MESH,
        )

    def x_arrival(k, ch):
        q = lax.rem(g + k, groups)
        rows = pl.ds(pl.multiple_of(ch * ROWS, ROWS), ROWS)
        block = xb.at[pl.ds(q * local, local), rows]
        return pltpu.make_async_remote_copy(
            src_ref=block, dst_ref=block, send_sem=x_send.at[k, ch], recv_sem=x_recv.at[q, ch],
            device_id=(q, d), device_id_type=MESH,
        )

    for k in range(1, groups):
        lev_copy(k).start()
    for ch in range(chunks):
        for k in range(1, groups):
            x_copy(k, ch).start()

    lev[g] = levels[...]
    for k in range(1, groups):
        q = lax.rem(g + k, groups)
        pltpu.make_async_remote_copy(
            src_ref=lev.at[q], dst_ref=lev.at[q], send_sem=lev_send.at[k], recv_sem=lev_recv.at[q],
            device_id=(q, d), device_id_type=MESH,
        ).wait_recv()
    lev_eye = lax.broadcasted_iota(jnp.int32, (local, local), 0) == lax.broadcasted_iota(
        jnp.int32, (local, local), 1
    )
    for h in range(groups):
        for axis in range(3):
            lev_row = lev[h, axis:axis + 1, :].astype(F32)
            lev_col = jnp.sum(jnp.where(lev_eye, lev_row, 0.0), axis=1, keepdims=True)
            lbc[axis, pl.ds(h * local, local), :] = jnp.broadcast_to(lev_col, (local, 128))
    lev_out[...] = lbc[:, pl.ds(pl.multiple_of(g * local, 8), local), :]
    prod[...] = jnp.zeros_like(prod)
    own_copy.wait()
    flat = xb.reshape(grids * subs, half)

    def gram_chunk(ch, carry):
        for k in range(1, groups):
            x_arrival(k, ch).wait_recv()
        lev0, lev1, lev2 = lbc[0], lbc[1], lbc[2]
        total = jnp.zeros(prod.shape, F32)
        for pair in range(0, ROWS, 2):
            parts = []
            for k in range(pair, pair + 2):
                s = ch * ROWS + k
                x = flat[pl.ds(s, grids, stride=subs), :]
                keep = (
                    (lev0 >= (s // 16).astype(F32))
                    & (lev1 >= lax.rem(s // 4, 4).astype(F32))
                    & (lev2 >= float(k % 4))
                )
                keep = jnp.concatenate([keep] * (half // 128), axis=1) if half > 128 else keep
                parts.append(jnp.where(keep, x, 0.0))
            y = split3(jnp.concatenate(parts, axis=1))
            total += lax.dot_general(y, y, (((1,), (1,)), ((), ())), preferred_element_type=F32)
        prod[...] += total
        return carry

    lax.fori_loop(0, chunks, gram_chunk, 0)

    part = prod[2 * grids:, :] + prod[grids:2 * grids, :] + prod[:grids, :]
    part = part[:, 2 * grids:] + part[:, grids:2 * grids] + part[:, :grids]
    value = jnp.concatenate([part, jnp.zeros((grids, 128 - grids), F32)], axis=1)
    fold = grids // 2
    value = value[:fold] + pltpu.roll(value[fold:], 64, 1)

    copies = []
    for t, (n, mine, device) in enumerate(members):
        buf, send, recv = slots[t], s_send[t], s_recv[t]
        buf[mine] = value
        for k in range(1, n):
            q = lax.rem(mine + k, n)
            copy = pltpu.make_async_remote_copy(
                src_ref=buf.at[mine], dst_ref=buf.at[mine], send_sem=send.at[k], recv_sem=recv.at[mine],
                device_id=device(q), device_id_type=MESH,
            )
            copy.start()
            copies.append(copy)
        for k in range(1, n):
            q = lax.rem(mine + k, n)
            pltpu.make_async_remote_copy(
                src_ref=buf.at[q], dst_ref=buf.at[q], send_sem=send.at[k], recv_sem=recv.at[q],
                device_id=device(q), device_id_type=MESH,
            ).wait_recv()
        value = buf[0]
        for q in range(1, n):
            value = value + buf[q]

    left = lax.broadcasted_iota(jnp.int32, (fold, 128), 1) < 64
    value = jnp.concatenate(
        [jnp.where(left, value, 0.0), jnp.where(left, pltpu.roll(value, 64, 1), 0.0)], axis=0
    )

    row = lax.broadcasted_iota(jnp.int32, (grids, 128), 0)
    col = lax.broadcasted_iota(jnp.int32, (grids, 128), 1)
    eye = row == col
    diag = jnp.where(eye, value, 0.0)
    diag_col = jnp.sum(diag, axis=1, keepdims=True) + 1e-06
    diag_row = jnp.sum(diag, axis=0, keepdims=True) + 1e-06
    scale_col = 1.0 / jnp.sqrt(diag_col)
    scale_row = 1.0 / jnp.sqrt(diag_row)
    system = scale_col * value * scale_row + jnp.where(eye, 0.1, 0.0)
    system = jnp.where(col == grids, jnp.sqrt(diag_col), jnp.where(col < grids, system, 0.0))
    for first in range(0, grids, BLOCK):
        width = min(BLOCK, grids - first)
        rows = [system[first + j:first + j + 1, :] for j in range(width)]
        cols = [
            jnp.broadcast_to(system[:, first + j:first + j + 1], (grids, 128)) for j in range(width)
        ]
        for j in range(width):
            k = first + j
            inverse = 1.0 / cols[j][k:k + 1, :]
            factor = jnp.where(row == k, 0.0, cols[j] * inverse)
            for m in range(j + 1, width):
                cols[m] = cols[m] - factor * cols[m][k:k + 1, :]
                rows[m] = rows[m] - factor[first + m:first + m + 1, :] * rows[j]
            system = system - factor * rows[j]
    final = jnp.sum(jnp.where(eye, system, 0.0), axis=1, keepdims=True)
    coef = scale_col * (system[:, grids:grids + 1] / final)
    coef_wide = jnp.broadcast_to(coef, (grids, 128))
    coef_out[...] = jnp.sum(jnp.where(eye, coef_wide, 0.0), axis=0, keepdims=True)[:, :grids]

    piece = subs // PIECES

    def c_copy(slot, k, p):
        block = cbuf.at[slot, pl.ds(p * piece, piece)]
        return pltpu.make_async_remote_copy(
            src_ref=block, dst_ref=block, send_sem=c_send.at[k, p], recv_sem=c_recv.at[slot, p],
            device_id=(lax.rem(g + k, groups), d), device_id_type=MESH,
        )

    for p in range(PIECES):
        sub = lax.broadcasted_iota(jnp.int32, (piece, half), 0) + p * piece
        dig0, dig1, dig2 = digits_of(sub)
        acc = jnp.zeros((piece, half), F32)
        for i in range(grids):
            keep = (
                (lbc[0, i:i + 1, 0:1] >= dig0)
                & (lbc[1, i:i + 1, 0:1] >= dig1)
                & (lbc[2, i:i + 1, 0:1] >= dig2)
            )
            acc += jnp.where(keep, coef_wide[i:i + 1, 0:1], 0.0) * xb[i, p * piece:(p + 1) * piece]
        cbuf[g, p * piece:(p + 1) * piece] = acc
        for k in range(1, groups):
            c_copy(g, k, p).start()
    for p in range(PIECES):
        for k in range(1, groups):
            c_copy(lax.rem(g + k, groups), k, p).wait_recv()
    for h in range(groups):
        comb_out[:, h * half:(h + 1) * half] = cbuf[h]

    for copy in copies:
        copy.wait_send()
    for k in range(1, groups):
        lev_copy(k).wait_send()
        for ch in range(chunks):
            x_copy(k, ch).wait_send()
        for p in range(PIECES):
            c_copy(g, k, p).wait_send()


def split3_rows(x):
    hi = x.astype(jnp.bfloat16).astype(F32)
    rest = x - hi
    mid = rest.astype(jnp.bfloat16).astype(F32)
    return jnp.concatenate([hi, mid, rest - mid], axis=0).astype(jnp.bfloat16)


def layout_of(groups, radices, g, d):
    members = []
    stride = 1
    for t, r in enumerate(radices):
        digit = lax.rem(d // stride, r)
        base = d - digit * stride
        if t == 0:
            n = groups * r
            mine = g * r + digit
            device = functools.partial(lambda b, r_, q: (q // r_, b + lax.rem(q, r_)), base, r)
        else:
            n = r
            mine = digit
            device = functools.partial(lambda b, st, q: (g, b + q * st), base, stride)
        members.append((n, mine, device))
        stride *= r
    return members


def spread_out(members, t, buf, send, recv, value):
    n, mine, device = members[t]
    buf[mine] = value
    copies = []
    for k in range(1, n):
        copy = pltpu.make_async_remote_copy(
            src_ref=buf.at[mine], dst_ref=buf.at[mine], send_sem=send.at[k], recv_sem=recv.at[mine],
            device_id=device(lax.rem(mine + k, n)), device_id_type=MESH,
        )
        copy.start()
        copies.append(copy)
    return copies


def gather_in(members, t, buf, send, recv):
    n, mine, device = members[t]
    for k in range(1, n):
        q = lax.rem(mine + k, n)
        pltpu.make_async_remote_copy(
            src_ref=buf.at[q], dst_ref=buf.at[q], send_sem=send.at[k], recv_sem=recv.at[q],
            device_id=device(q), device_id_type=MESH,
        ).wait_recv()


def total_of(buf, first, last):
    value = buf[first]
    for q in range(first + 1, last):
        value = value + buf[q]
    return value


def pack(square):
    local = square.shape[0]
    wide = jnp.concatenate([square, jnp.zeros((local, 128 - local), F32)], axis=1)
    out = wide[:8]
    for b in range(1, local // 8):
        out = out + pltpu.roll(wide[8 * b:8 * b + 8], SLOT * b, 1)
    return out


def unpack(packed, local):
    rows = [packed] + [pltpu.roll(packed, 128 - SLOT * b, 1) for b in range(1, local // 8)]
    wide = jnp.concatenate(rows, axis=0)
    return jnp.where(lax.broadcasted_iota(jnp.int32, (local, 128), 1) < local, wide, 0.0)


def folded(products, n):
    part = products[2 * n:, :] + products[n:2 * n, :] + products[:n, :]
    return part[:, 2 * n:] + part[:, n:2 * n] + part[:, :n]


def outer(a, b):
    return lax.dot_general(a, b, (((1,), (1,)), ((), ())), preferred_element_type=F32)


def count_dot(a, b):
    bf16 = jnp.bfloat16
    return jnp.dot(a.astype(bf16), b.astype(bf16), preferred_element_type=F32)


def below(n, m, flip):
    r = lax.broadcasted_iota(jnp.int32, (n, m), 0)
    c = lax.broadcasted_iota(jnp.int32, (n, m), 1)
    return jnp.where((r < c) if flip else (r > c), 1.0, 0.0)


def solve(value, grids):
    row = lax.broadcasted_iota(jnp.int32, (grids, 128), 0)
    col = lax.broadcasted_iota(jnp.int32, (grids, 128), 1)
    eye = row == col
    diag = jnp.where(eye, value, 0.0)
    diag_col = jnp.sum(diag, axis=1, keepdims=True) + 1e-06
    diag_row = jnp.sum(diag, axis=0, keepdims=True) + 1e-06
    scale_col = 1.0 / jnp.sqrt(diag_col)
    scale_row = 1.0 / jnp.sqrt(diag_row)
    system = scale_col * value * scale_row + jnp.where(eye, 0.1, 0.0)
    system = jnp.where(col == grids, jnp.sqrt(diag_col), jnp.where(col < grids, system, 0.0))
    for first in range(0, grids, BLOCK):
        width = min(BLOCK, grids - first)
        rows = [system[first + j:first + j + 1, :] for j in range(width)]
        cols = [
            jnp.broadcast_to(system[:, first + j:first + j + 1], (grids, 128)) for j in range(width)
        ]
        for j in range(width):
            k = first + j
            inverse = 1.0 / cols[j][k:k + 1, :]
            factor = jnp.where(row == k, 0.0, cols[j] * inverse)
            for m in range(j + 1, width):
                cols[m] = cols[m] - factor * cols[m][k:k + 1, :]
                rows[m] = rows[m] - factor[first + m:first + m + 1, :] * rows[j]
            system = system - factor * rows[j]
    final = jnp.sum(jnp.where(eye, system, 0.0), axis=1, keepdims=True)
    coef = scale_col * (system[:, grids:grids + 1] / final)
    return jnp.broadcast_to(coef, (grids, 128)), eye


def parts_of(x):
    hi = x.astype(jnp.bfloat16)
    left = x - hi.astype(F32)
    mid = left.astype(jnp.bfloat16)
    return hi, mid, (left - mid.astype(F32)).astype(jnp.bfloat16)


def places_of(keep, across):
    n, m = keep.shape
    if across:
        totals = count_dot(jnp.ones((n, n), F32), keep)
        pos = count_dot(below(n, n, False), keep) + count_dot(totals, below(m, m, True))
    else:
        totals = count_dot(keep, jnp.ones((m, m), F32))
        pos = count_dot(below(n, n, False), totals) + count_dot(keep, below(m, m, True))
    return jnp.where(keep > 0.0, pos, -1.0)


def sparse_kernel(groups, radices, local, subs, cap, surplus, levels, comb_out, coef_out, lev_out, fits_out, *scratch):
    stages = len(radices)
    (xh, xm, xs, ym, pm, csend, crecv, posm, lev, prod, local_sem, m_sem, lev_sem, x_send,
     x_recv, fits) = scratch[:16]
    rest = [scratch[16 + m * stages:16 + (m + 1) * stages] for m in range(6)]
    slots, s_send, s_recv, own_slots, o_send, o_recv = rest
    grids = groups * local
    half = xh.shape[-1]
    rows_all = local * subs
    chunks = cap // STEP
    bf16 = jnp.bfloat16
    g = lax.axis_index("grp")
    d = lax.axis_index("dom")
    other = 1 - g
    members = layout_of(groups, radices, g, d)

    cells = [pl.ds(pl.multiple_of(h * half, half), half) for h in (other, g)]
    lev_load = pltpu.make_async_copy(levels, lev.at[g], local_sem.at[2])
    lev_load.start()
    loads = [pltpu.make_async_copy(surplus.at[:, :, cells[h]], xh.at[h], local_sem.at[h]) for h in range(2)]
    for load in loads:
        load.start()
    turns = [pltpu.make_async_copy(surplus.at[i], xm.at[:, i, :], m_sem.at[i]) for i in range(local)]

    barrier = pltpu.get_barrier_semaphore()
    count = 0
    for n, mine, device in members:
        for k in range(1, n):
            pl.semaphore_signal(barrier, inc=1, device_id=device(lax.rem(mine + k, n)), device_id_type=MESH)
            count += 1

    def lev_wide(h):
        eye = lax.broadcasted_iota(jnp.int32, (local, local), 0) == lax.broadcasted_iota(jnp.int32, (local, local), 1)
        out = []
        for axis in range(3):
            lev_row = lev[h, axis:axis + 1, :].astype(F32)
            lev_col = jnp.sum(jnp.where(eye, lev_row, 0.0), axis=1, keepdims=True)
            out.append(jnp.broadcast_to(lev_col, (local, 128)))
        return out

    def kept_by(wide):
        digits = digits_of(lax.broadcasted_iota(jnp.int32, (local, 128), 1))
        keep = jnp.ones((local, 128), F32)
        for axis in range(3):
            keep = jnp.where(wide[axis] >= digits[axis], keep, 0.0)
        return keep

    lev_load.wait()
    wide = lev_wide(g)
    for axis in range(3):
        lev_out[axis] = wide[axis]
    keep = kept_by(wide)
    own_count = jnp.sum(keep)
    pos = places_of(keep, True)
    pos_far = pltpu.roll(pos, 64, 1)
    low = lax.broadcasted_iota(jnp.int32, (1, 128), 1) < subs
    pos_rows = [jnp.where(low, pos[i:i + 1], pos_far[i + 1:i + 2]) for i in range(0, local, 128 // subs)]

    def split_half(h):
        flat = xh.at[h].reshape(rows_all, half)
        for i in range(0, rows_all, 256):
            for m, part in enumerate(parts_of(flat[i:i + 256, :])):
                xs[h, i:i + 256, m * half:(m + 1) * half] = part

    loads[0].wait()
    for turn in turns:
        turn.start()
    split_half(0)
    def x_copy(h, ch):
        rows = pl.ds(pl.multiple_of(ch * STEP, STEP), STEP)
        return pltpu.make_async_remote_copy(
            src_ref=csend.at[h, rows], dst_ref=crecv.at[h, rows], send_sem=x_send.at[h, ch], recv_sem=x_recv.at[h, ch],
            device_id=(other, d), device_id_type=MESH,
        )

    index = lax.broadcasted_iota(jnp.int32, (256, 128), 0).astype(F32)

    def gather_rows(h, first):
        want = index + float(first)
        acc = jnp.zeros((256, 3 * half), F32)
        for m in range(0, len(pos_rows), 2):
            picks = [jnp.where(want == p, 1.0, 0.0).astype(bf16) for p in pos_rows[m:m + 2]]
            acc += jnp.dot(
                jnp.concatenate(picks, axis=1), xs[h, m * 128:m * 128 + 256, :], preferred_element_type=F32
            )
        csend[h, first:first + 256, :] = acc[:, :half] + acc[:, half:2 * half] + acc[:, 2 * half:]

    def depart(h, first, last):
        for ch in range(first // STEP, last // STEP):
            x_copy(h, ch).start()

    gather_rows(0, 0)
    pl.semaphore_wait(barrier, count)
    lev_copy = pltpu.make_async_remote_copy(
        src_ref=lev.at[g], dst_ref=lev.at[g], send_sem=lev_sem.at[0], recv_sem=lev_sem.at[1],
        device_id=(other, d), device_id_type=MESH,
    )
    lev_copy.start()
    depart(0, 0, 256)
    for first in range(256, cap, 256):
        gather_rows(0, first)
        depart(0, first, first + 256)
    loads[1].wait()
    split_half(1)
    gather_rows(1, 0)
    depart(1, 0, EARLY)

    for turn in turns:
        turn.wait()
    prod[...] = jnp.zeros_like(prod)

    def own_gram(ch, carry):
        total = jnp.zeros(prod.shape, F32)
        for k in range(ROWS):
            s = ch * ROWS + k
            own = (
                (lev_out[0] >= (s // 16).astype(F32))
                & (lev_out[1] >= lax.rem(s // 4, 4).astype(F32))
                & (lev_out[2] >= float(k % 4))
            )
            own = jnp.concatenate([own] * (groups * half // 128), axis=1)
            x = jnp.where(own, xm[s], 0.0)
            xm[s] = x
            y = split3_rows(x)
            ym[s] = jnp.where(g == 0, y[:, :half], y[:, half:])
            total += outer(y, y)
        prod[...] += total
        return carry

    lax.fori_loop(0, subs // ROWS, own_gram, 0)

    lev_copy.wait_recv()
    keep = kept_by(lev_wide(other))
    fits[0, 0] = jnp.where(jnp.maximum(own_count, jnp.sum(keep)) <= float(cap), 1, 0)
    fits_copy = pltpu.make_async_copy(fits, fits_out, local_sem.at[3])
    fits_copy.start()
    pos = places_of(keep, True)
    for s in range(subs):
        posm[s * local:(s + 1) * local, :] = jnp.broadcast_to(pos[:, s:s + 1], (local, 128))

    copies = spread_out(members, 0, own_slots[0], o_send[0], o_recv[0], pack(folded(prod[...], local)))

    def parts_at(h, first):
        return jnp.concatenate(parts_of(crecv[h, first:first + 256, :]), axis=1)

    def placed(where, first, parts, n):
        lane = lax.broadcasted_iota(jnp.int32, (n, 128), 1).astype(F32) + float(first)
        picks = [jnp.where(where == lane + float(c), 1.0, 0.0).astype(bf16) for c in range(0, 256, 128)]
        y = jnp.dot(jnp.concatenate(picks, axis=1), parts, preferred_element_type=F32)
        return y[:, :half] + y[:, half:2 * half] + y[:, 2 * half:]

    def arrive(h, first):
        for ch in range(first // STEP, (first + 256) // STEP):
            x_copy(h, ch).wait_recv()

    last = cap - 256
    for first in range(0, last, 256):
        arrive(0, first)
        parts = parts_at(0, first)

        for at in range(0, rows_all, BAND):
            y = placed(posm[at:at + BAND, :], first, parts, BAND)
            pm[g, at:at + BAND, :] = y if first == 0 else pm[g, at:at + BAND, :] + y

    arrive(0, last)
    parts = parts_at(0, last)
    total = jnp.zeros((3 * local, 3 * local), F32)
    for at in range(0, rows_all, BAND):
        y = placed(posm[at:at + BAND, :], last, parts, BAND)
        if last > 0:
            y = y + pm[g, at:at + BAND, :]
        pm[g, at:at + BAND, :] = y
        for k in range(0, BAND // local, 2):
            s = at // local + k
            theirs = split3_rows(
                jnp.concatenate([y[(k + j) * local:(k + j + 1) * local] for j in range(2)], axis=1)
            )
            ours = jnp.concatenate([ym[s], ym[s + 1]], axis=1)
            total += outer(jnp.where(g == 0, ours, theirs), jnp.where(g == 0, theirs, ours))

    def finish_late():
        for first in range(0, cap, 256):
            arrive(1, first)
            parts = parts_at(1, first)
            for at in range(0, rows_all, BAND):
                y = placed(posm[at:at + BAND, :], first, parts, BAND)
                pm[other, at:at + BAND, :] = y if first == 0 else pm[other, at:at + BAND, :] + y

    value = pack(folded(total, local))
    for t in range(stages):
        copies += spread_out(members, t, slots[t], s_send[t], s_recv[t], value)
        if t == 0:
            depart(1, EARLY, 256)
            for first in range(256, cap, 256):
                gather_rows(1, first)
                depart(1, first, first + 256)
        gather_in(members, t, own_slots[t], o_send[t], o_recv[t])
        n = members[t][0]
        if t == 0:
            own_total = jnp.concatenate(
                [total_of(own_slots[0], 0, n // 2), total_of(own_slots[0], n // 2, n)], axis=0
            )
        else:
            own_total = total_of(own_slots[t], 0, n)
        if t + 1 < stages:
            copies += spread_out(members, t + 1, own_slots[t + 1], o_send[t + 1], o_recv[t + 1], own_total)
        else:
            finish_late()
        gather_in(members, t, slots[t], s_send[t], s_recv[t])
        value = total_of(slots[t], 0, members[t][0])

    upper = unpack(value, local)
    square = jnp.concatenate([upper, jnp.zeros((128 - local, 128), F32)], axis=0)
    lower = square.T[:local]
    value = jnp.concatenate(
        [
            unpack(own_total[:8], local) + pltpu.roll(upper, local, 1),
            lower + pltpu.roll(unpack(own_total[8:], local), local, 1),
        ],
        axis=0,
    )
    coef_wide, eye = solve(value, grids)
    coef_out[...] = jnp.sum(jnp.where(eye, coef_wide, 0.0), axis=0, keepdims=True)[:, :grids]

    ours = jnp.where(g == 0, coef_wide[:local], coef_wide[local:])
    theirs = jnp.where(g == 0, coef_wide[local:], coef_wide[:local])
    if half > 128:
        ours, theirs = [jnp.concatenate([w] * (half // 128), axis=1) for w in (ours, theirs)]
    for h in range(groups):
        for first in range(0, subs, 8):
            at = first * local
            acc = xm[first:first + 8, :, h * half:(h + 1) * half] * ours[None] + (
                pm[h, at:at + 8 * local, :].reshape(8, local, half) * theirs[None]
            )
            comb_out[first:first + 8, h * half:(h + 1) * half] = jnp.sum(acc, axis=1)

    fits_copy.wait()
    for copy in copies:
        copy.wait_send()
    lev_copy.wait_send()
    for h in range(2):
        for ch in range(chunks):
            x_copy(h, ch).wait_send()


def spread(combined, coef, lev, updated, coef_out, block, sems):
    local, subs, cells = updated.shape
    coef_out[...] = coef[...]
    dig0, dig1, dig2 = digits_of(lax.broadcasted_iota(jnp.int32, (subs, 128), 0))
    copies = []
    for i in range(local):
        keep = (lev[0, i:i + 1, :] >= dig0) & (lev[1, i:i + 1, :] >= dig1) & (lev[2, i:i + 1, :] >= dig2)
        for c in range(0, cells, 128):
            block[i, :, c:c + 128] = jnp.where(keep, combined[:, c:c + 128], 0.0)
        if (i + 1) % SPREAD == 0 or i + 1 == local:
            n = len(copies)
            part = pl.ds(n * SPREAD, i + 1 - n * SPREAD)
            copy = pltpu.make_async_copy(block.at[part], updated.at[part], sems.at[n])
            copy.start()
            copies.append(copy)
    for copy in copies:
        copy.wait()


def dense_call(groups, radices, surplus, levels, identity):
    local, subs, cells = surplus.shape
    grids = groups * local
    half = cells // groups
    sizes = [groups * r if t == 0 else r for t, r in enumerate(radices)]
    dma = pltpu.SemaphoreType.DMA
    chunks = subs // ROWS
    return pl.pallas_call(
        functools.partial(kernel, groups, radices, local, subs),
        out_shape=(
            jax.ShapeDtypeStruct((subs, cells), F32),
            jax.ShapeDtypeStruct((1, grids), F32),
            jax.ShapeDtypeStruct((3, local, 128), F32),
        ),
        in_specs=[pl.BlockSpec(memory_space=pltpu.HBM), pl.BlockSpec(memory_space=pltpu.VMEM)],
        out_specs=tuple(pl.BlockSpec(memory_space=pltpu.VMEM) for _ in range(3)),
        scratch_shapes=[
            pltpu.VMEM((grids, subs, half), F32),
            pltpu.VMEM((groups, 3, local), jnp.int32),
            pltpu.VMEM((3, grids, 128), F32),
            pltpu.VMEM((3 * grids, 3 * grids), F32),
            pltpu.VMEM((groups, subs, half), F32),
            dma(()), dma((groups,)), dma((groups,)),
            dma((groups, chunks)), dma((groups, chunks)), dma((groups, PIECES)), dma((groups, PIECES)),
        ]
        + [pltpu.VMEM((n, grids // 2, 128), F32) for n in sizes]
        + [dma((n,)) for n in sizes]
        + [dma((n,)) for n in sizes],
        compiler_params=pltpu.CompilerParams(
            collective_id=identity, has_side_effects=True, vmem_limit_bytes=VMEM_BYTES
        ),
    )(surplus, levels)


def sparse_call(groups, radices, surplus, levels, identity):
    local, subs, cells = surplus.shape
    grids = groups * local
    half = cells // groups
    cap = local * subs // 3 // 256 * 256
    chunks = cap // STEP
    sizes = [groups * r if t == 0 else r for t, r in enumerate(radices)]
    dma = pltpu.SemaphoreType.DMA
    return pl.pallas_call(
        functools.partial(sparse_kernel, groups, radices, local, subs, cap),
        out_shape=(
            jax.ShapeDtypeStruct((subs, cells), F32),
            jax.ShapeDtypeStruct((1, grids), F32),
            jax.ShapeDtypeStruct((3, local, 128), F32),
            jax.ShapeDtypeStruct((1, 1), jnp.int32),
        ),
        in_specs=[pl.BlockSpec(memory_space=pltpu.HBM), pl.BlockSpec(memory_space=pltpu.HBM)],
        out_specs=tuple(pl.BlockSpec(memory_space=pltpu.VMEM) for _ in range(3))
        + (pl.BlockSpec(memory_space=pltpu.HBM),),
        scratch_shapes=[
            pltpu.VMEM((2, local, subs, half), F32),
            pltpu.VMEM((subs, local, cells), F32),
            pltpu.VMEM((2, local * subs, 3 * half), jnp.bfloat16),
            pltpu.VMEM((subs, 3 * local, half), jnp.bfloat16),
            pltpu.VMEM((2, local * subs, half), F32),
            pltpu.VMEM((2, cap, half), F32),
            pltpu.VMEM((2, cap, half), F32),
            pltpu.VMEM((local * subs, 128), F32),
            pltpu.VMEM((groups, 3, local), jnp.int32),
            pltpu.VMEM((3 * local, 3 * local), F32),
            dma((4,)), dma((local,)), dma((2,)), dma((2, chunks)), dma((2, chunks)),
            pltpu.SMEM((1, 1), jnp.int32),
        ]
        + [pltpu.VMEM((n, 8, 128), F32) for n in sizes]
        + [dma((n,)) for n in sizes]
        + [dma((n,)) for n in sizes]
        + [pltpu.VMEM((n, 8 if t == 0 else 16, 128), F32) for t, n in enumerate(sizes)]
        + [dma((n,)) for n in sizes]
        + [dma((n,)) for n in sizes],
        compiler_params=pltpu.CompilerParams(
            collective_id=identity, has_side_effects=True, vmem_limit_bytes=VMEM_BYTES
        ),
    )(surplus, levels)


def shards(groups, domains, surplus, levels):
    local, subs, cells = surplus.shape
    grids = groups * local
    radices = radices_of(domains)
    flipped = levels.T
    *found, fits = sparse_call(groups, radices, surplus, flipped, 0)
    combined, coefficients, lev_wide = lax.cond(
        fits[0, 0] == 1,
        lambda *kept: tuple(kept[2:]),
        lambda *kept: tuple(dense_call(groups, radices, kept[0], kept[1], 1)),
        surplus, flipped, *found,
    )
    updated, coefficients = pl.pallas_call(
        spread,
        out_shape=(
            jax.ShapeDtypeStruct((local, subs, cells), F32),
            jax.ShapeDtypeStruct((1, grids), F32),
        ),
        in_specs=[pl.BlockSpec(memory_space=pltpu.VMEM)] * 3,
        out_specs=(pl.BlockSpec(memory_space=pl.ANY), pl.BlockSpec(memory_space=pltpu.VMEM)),
        scratch_shapes=[pltpu.VMEM((local, subs, cells), F32), pltpu.SemaphoreType.DMA((-(-local // SPREAD),))],
        compiler_params=pltpu.CompilerParams(vmem_limit_bytes=VMEM_BYTES),
    )(combined, coefficients, lev_wide)
    return (updated, coefficients.reshape(grids))


def solution(mesh):
    placed = (P("grp", None, "dom"), P("grp", None))
    return jax.shard_map(
        functools.partial(shards, mesh.shape["grp"], mesh.shape["dom"]),
        mesh=mesh, in_specs=placed, out_specs=(P("grp", None, "dom"), P()), check_vma=False,
    )
```
